128 devices in a mesh: grp: 8 (over y, core), mem: 16 (over x, z).
Axes of the slice: x: 4, y: 4, z: 4, core: 2. Of those that a mesh axis runs over, the one named last changes fastest.
Arguments:
- factors: bfloat16 [256, 288, 1792], P(('grp', 'mem')), may hold values from -3 to 3
- screen: int32 [128, 18], P(('grp', 'mem')), may hold values from 0 to 1, as said below
Outputs:
- exchange_matrix: float32 [1792, 1792], P(('grp', 'mem'))
The draws below stay inside these ranges and needn't reach their ends.
Inputs may be any that keep to these rules, and one draw needn't show every extreme that they name: screen[b, j] is 1 where auxiliary block b and occupied block j survive screening; every auxiliary block keeps at least one occupied block.
All inputs are finite; a program needn't handle non-finite values.
Results may differ from the reference program's by a relative error of at most 0.0003.
Values may be sent and summed in bfloat16 or wider, within the bound.
A program may use at most 128 MiB of HBM per device.

```python
import jax
import jax.numpy as jnp
from jax import lax

NBF = 1792
NOCC = 288
NOB = 18
NAB = 128
NAUX = 256


def draw_screen(key, part):
    count_key = jax.random.fold_in(key, 11)
    shuffle_key = jax.random.fold_in(key, 23)
    kept_count = jax.random.randint(count_key, (NAB, 1), 1, NOB + 1)
    row_keys = jax.random.split(shuffle_key, NAB)

    def shuffle_row(row_key):
        return jax.random.permutation(row_key, NOB)
    shuffled = jax.vmap(shuffle_row)(row_keys)
    position = jnp.argsort(shuffled, axis=1)
    return (position < kept_count).astype(jnp.int32)


def with_spikes(array, own_key, source, target, blocks, factor):
    def block_of(dim):
        return (jnp.arange(array.shape[dim]) // (array.shape[dim] // blocks)).reshape((-1,) + (1,) * (array.ndim - 1 - dim))

    near = jax.random.permutation(own_key, blocks)[block_of(target)]
    second = (block_of(target) + blocks // 2) % blocks
    return jnp.where((block_of(source) == near) | (block_of(source) == second), factor * array, array)


def steps_of(own_key, extent, pieces, low, top_value):
    def one(axis_at, parts):
        draws = jax.random.uniform(jax.random.fold_in(jax.random.fold_in(own_key, 6), axis_at), (parts,), jnp.float32, low / len(pieces), top_value / len(pieces))
        return jnp.repeat(jnp.exp(draws), extent[axis_at] // parts).reshape((-1,) + (1,) * (len(extent) - axis_at - 1))

    level = one(*pieces[0])
    for cut in pieces[1:]:
        level = level * one(*cut)
    return level


def bell_draw_with(own_key, dims, width, most, cuts, heavy, dtype=jnp.bfloat16):
    values = width * jax.random.normal(own_key, dims, jnp.float32)
    if cuts:
        values = values * steps_of(own_key, dims, cuts, -0.22, 0.18)
    return jnp.clip(with_spikes(values, jax.random.fold_in(own_key, 3), *heavy), -most, most).astype(dtype)


def setup_inputs(seed: int = 0) -> dict:
    keys = jax.random.split(jax.random.key(seed), 3)
    factors = bell_draw_with(keys[0], (NAUX, NOCC, NBF), 0.05, 3.0, ((0, 128),), (0, 2, 128, 5.5))
    screen = draw_screen(jax.random.fold_in(keys[2], 71), 0)
    return {"factors": factors, "screen": screen}


def reference(factors, screen):
    total_aux, occ_count, basis = factors.shape
    block_count, occ_blocks = screen.shape
    aux_rows = total_aux // block_count
    occ_width = occ_count // occ_blocks
    grouped = factors.reshape(block_count, aux_rows, occ_blocks, occ_width, basis)

    def add_block(running, pair):
        block, flags = pair
        masked = block * flags.astype(jnp.bfloat16)[None, :, None, None]
        flat_rows = masked.reshape(-1, basis)
        return running + jnp.dot(flat_rows.T, flat_rows, preferred_element_type=jnp.float32), None

    result, _ = lax.scan(add_block, jnp.zeros((basis, basis), jnp.float32), (grouped, screen))
    return result
```

```python
import functools

import jax
import jax.numpy as jnp
from jax import lax
from jax.experimental import pallas as pl
from jax.experimental.pallas import tpu as pltpu
from jax.sharding import PartitionSpec as P

LANES = 128
TOP = 32767.0
SIDE = 4
HEAD = 16
MESH = pl.DeviceIdType.MESH
ORDERS = ("yxz", "zxy", "xyz", "yxz", "zxy", "xyz", "yxz")


def kernel(
    members, width, orders, pieces,
    x_ref, screen_ref, out_ref,
    both, turned, total, first_sum, second_sum,
    out_one, in_one, out_two, in_two, out_three, in_three, out_four, in_four,
    load_sem, pair_send, pair_recv, one_send, one_recv, two_send, two_recv,
    three_send, three_recv, four_send, four_recv,
):
    depth, basis = x_ref.shape
    own = out_ref.shape[0]
    half = basis // 2
    parts = len(orders)
    occ_blocks = screen_ref.shape[1]
    grp, mem = lax.axis_index("grp"), lax.axis_index("mem")
    at = {"y": lax.div(grp, 2), "c": lax.rem(grp, 2), "x": lax.div(mem, SIDE), "z": lax.rem(mem, SIDE)}
    core = at["c"]

    def place(axis, d):
        return lax.rem(at[axis] + d, SIDE)

    def device(axis, d, flip=0):
        there = dict(at)
        if d:
            there[axis] = place(axis, d)
        if flip:
            there["c"] = 1 - core
        return (there["y"] * 2 + there["c"], there["x"] * SIDE + there["z"])

    last_axes = sorted({order[2] for order in orders})
    peers = [device("x", 0, 1)]
    for axis in "xyz":
        for d in range(1, SIDE):
            peers.append(device(axis, d))
            if axis in last_axes:
                peers.append(device(axis, d, 1))
    barrier = pltpu.get_barrier_semaphore()
    for other in peers:
        pl.semaphore_signal(barrier, inc=1, device_id=other, device_id_type=MESH)

    piece = depth // pieces
    loads = []
    for n in range(pieces):
        rows = pl.ds(n * piece, piece)
        loads.append(pltpu.make_async_copy(x_ref.at[rows], both.at[rows], load_sem.at[n]))
        loads[-1].start()

    total_rows = total.shape[1]
    for p in range(parts):
        total[p, basis:total_rows, :] = jnp.zeros((total_rows - basis, LANES), jnp.float32)
        tail = second_sum.shape[1]
        second_sum[p, tail - 16 : tail, :] = jnp.zeros((16, LANES), jnp.float32)

    def mask(j, carry):
        rows = pl.ds(pl.multiple_of(j * width, width), width)
        keep = screen_ref[0, lax.rem(j, occ_blocks)].astype(jnp.float32)
        both[rows, :] = (both[rows, :].astype(jnp.float32) * keep).astype(both.dtype)
        return carry

    pair = []
    partner = device("x", 0, 1)
    for n in range(pieces):
        loads[n].wait()
        lax.fori_loop(n * piece // width, (n + 1) * piece // width, mask, 0)
        if n == 0:
            pl.semaphore_wait(barrier, len(peers))
        pair.append(
            pltpu.make_async_remote_copy(
                src_ref=both.at[pl.ds(n * piece, piece)],
                dst_ref=both.at[pl.ds(depth + n * piece, piece)],
                send_sem=pair_send.at[n], recv_sem=pair_recv.at[n],
                device_id=partner, device_id_type=MESH,
            )
        )
        pair[-1].start()

    def turn(low, high):
        def one(m, carry):
            rows = pl.ds(pl.multiple_of(m * 256, 256), 256)
            for k in range(low, high, LANES):
                turned[rows, k : k + LANES] = both[k : k + LANES, rows].T
            return carry

        lax.fori_loop(0, basis // 256, one, 0)

    def multiply(tiles, low, high, fresh):
        tall = basis // 2
        columns = pl.ds(pl.multiple_of(core * half + tiles[0] * LANES, LANES), len(tiles) * LANES)

        def one(m, carry):
            rows = pl.ds(pl.multiple_of(m * tall, LANES), tall)
            value = jnp.dot(turned[rows, low:high], both[low:high, columns], preferred_element_type=jnp.float32)
            for n, p in enumerate(tiles):
                mine = value[:, n * LANES : (n + 1) * LANES]
                total[p, rows, :] = mine if fresh else total[p, rows, :] + mine
            return carry

        lax.fori_loop(0, 2, one, 0)

    def exponent(top):
        return jnp.floor(jnp.log(jnp.maximum(top, 1e-33)) * 1.4426950408889634) + 1.0

    def coded(value, power):
        return jnp.round(value * (jnp.exp2(-power) * TOP)).astype(jnp.int32).astype(jnp.int16)

    def put(ref, values):
        rows = lax.broadcasted_iota(jnp.int32, (HEAD, LANES), 0)
        head = jnp.zeros((HEAD, LANES), jnp.float32)
        for g, value in enumerate(values):
            power = exponent(jnp.max(jnp.abs(value), axis=0, keepdims=True))
            n = value.shape[0]
            ref[HEAD + g * n : HEAD + (g + 1) * n, :] = coded(value, power)
            head = jnp.where(rows == g, power, head)
        ref[0:HEAD, :] = head.astype(jnp.int32).astype(jnp.int16)

    def powers(ref):
        return jnp.exp2(ref[0:HEAD, :].astype(jnp.int32).astype(jnp.float32)) * (1.0 / TOP)

    def get(ref, scale, g, n):
        return ref[HEAD + g * n : HEAD + (g + 1) * n, :].astype(jnp.int32).astype(jnp.float32) * scale[g : g + 1, :]

    def group_rows(order):
        return 128 if order[0] == "z" else 112

    def load(p, order, block, c, g):
        if order[0] == "y":
            start = block * (8 * own * SIDE) + c * (4 * own * SIDE) + g * 112
            return total[p, pl.ds(pl.multiple_of(start, 8), 112), :]
        if order[0] == "x":
            starts = [(2 * g + n) * (8 * own * SIDE) + c * (4 * own * SIDE) + block * (own * SIDE) for n in range(2)]
            return jnp.concatenate([total[p, pl.ds(pl.multiple_of(s, 8), 56), :] for s in starts], axis=0)
        starts = [
            (2 * g + n) * (8 * own * SIDE) + c * (4 * own * SIDE) + m * (own * SIDE) + block * own
            for n in range(2) for m in range(SIDE)
        ]
        return jnp.concatenate([total[p, pl.ds(s, 16), :] for s in starts], axis=0)

    def second_block(p, order, j):
        if order[0] != "z" or order[1] == "y":
            n = 64 if order[0] == "z" else 56
            starts = [c * 4 * n + j * n for c in range(2)]
        else:
            n = 16
            starts = [c * 256 + m * 64 + j * n for c in range(2) for m in range(SIDE)]
        return jnp.concatenate([first_sum[p, pl.ds(pl.multiple_of(s, 8), n), :] for s in starts], axis=0)

    def copy(here, there, a, b, to):
        return pltpu.make_async_remote_copy(
            src_ref=here, dst_ref=there, send_sem=a, recv_sem=b, device_id=to, device_id_type=MESH,
        )

    def sized(order, groups):
        return pl.ds(0, HEAD + groups * group_rows(order))

    def copy_one(p, s):
        order = orders[p]
        run = sized(order, 2)
        return copy(out_one.at[p, s, run], in_one.at[p, s, run], one_send.at[p, s], one_recv.at[p, s],
                    device(order[0], (1, 3)[s]))

    def copy_two(p, s):
        order = orders[p]
        run = sized(order, 4)
        return copy(out_two.at[p, s, run], in_two.at[p, s, run], two_send.at[p, s], two_recv.at[p, s],
                    device(order[0], (1, 3)[s]))

    def copy_three(p, d):
        order = orders[p]
        run = sized(order, 1)
        return copy(out_three.at[p, d - 1, run], in_three.at[p, d - 1, run], three_send.at[p, d - 1],
                    three_recv.at[p, d - 1], device(order[1], d))

    def copy_four(p, d, flip):
        s = 2 * d + flip - 1
        return copy(out_four.at[p, s], in_four.at[p, s], four_send.at[p, s], four_recv.at[p, s],
                    device(orders[p][2], d, flip))

    def step_one(p):
        order = orders[p]
        block = place(order[0], 2)
        for s in range(2):
            put(out_one.at[p, s], [load(p, order, block, s, g) for g in range(2)])
            copy_one(p, s).start()

    def step_two(p):
        order = orders[p]
        n = group_rows(order)
        for s in range(2):
            copy_one(p, s).wait_recv()
            block = place(order[0], (1, 3)[s])
            scale = powers(in_one.at[p, s])
            values = []
            for c in range(2):
                for g in range(2):
                    value = load(p, order, block, c, g)
                    if c == s:
                        value = value + get(in_one.at[p, s], scale, g, n)
                    values.append(value)
            put(out_two.at[p, s], values)
            copy_two(p, s).start()

    def step_three(p):
        order = orders[p]
        n = group_rows(order)
        for s in range(2):
            copy_two(p, s).wait_recv()
        scales = [powers(in_two.at[p, s]) for s in range(2)]
        for c in range(2):
            for g in range(2):
                value = load(p, order, at[order[0]], c, g)
                for s in range(2):
                    value = value + get(in_two.at[p, s], scales[s], 2 * c + g, n)
                first_sum[p, (2 * c + g) * n : (2 * c + g + 1) * n, :] = value
        for d in range(1, SIDE):
            put(out_three.at[p, d - 1], [second_block(p, order, place(order[1], d))])
            copy_three(p, d).start()

    def last_rows(order, c, k):
        if order[0] == "z":
            return pl.ds(pl.multiple_of(c * 64 + k * 16, 8), 16)
        return pl.ds(c * 4 * own + k * own, 16)

    def step_four(p):
        order = orders[p]
        n = group_rows(order)
        value = second_block(p, order, at[order[1]])
        for d in range(1, SIDE):
            copy_three(p, d).wait_recv()
            ref = in_three.at[p, d - 1]
            value = value + get(ref, powers(ref), 0, n)
        second_sum[p, 0:n, :] = value
        rows = lax.broadcasted_iota(jnp.int32, (16, LANES), 0)
        for d in range(SIDE):
            for flip in range(2):
                if d or flip:
                    c = 1 - core if flip else core
                    value = second_sum[p, last_rows(order, c, place(order[2], d)), :]
                    top = jnp.max(jnp.where(rows < own, jnp.abs(value), 0.0), axis=0, keepdims=True)
                    power = exponent(top)
                    code = jnp.round(value * (jnp.exp2(-power) * TOP))
                    code = jnp.where(rows < own, code, power)
                    out_four[p, 2 * d + flip - 1] = code.astype(jnp.int32).astype(jnp.int16)
                    copy_four(p, d, flip).start()

    def step_five(p):
        order = orders[p]
        for flip in range(2):
            c = 1 - core if flip else core
            value = None
            if not flip:
                value = second_sum[p, last_rows(order, core, at[order[2]]), :]
            for d in range(SIDE):
                if d or flip:
                    copy_four(p, d, flip).wait_recv()
                    code = in_four[p, 2 * d + flip - 1].astype(jnp.int32).astype(jnp.float32)
                    term = code * (jnp.exp2(code[own : own + 1, :]) * (1.0 / TOP))
                    value = term if value is None else value + term
            columns = pl.ds(pl.multiple_of(c * half + p * LANES, LANES), LANES)
            out_ref[:, columns] = value[0:own, :]

    early = depth // LANES * LANES
    chunks = [list(range(p, min(p + 2, parts))) for p in range(0, parts, 2)]
    turn(0, early)
    for tiles in chunks:
        multiply(tiles, 0, early, True)
    done = early
    for n in range(pieces):
        pair[n].wait_recv()
        ready = (depth + (n + 1) * piece) // LANES * LANES
        if ready > done:
            turn(done, ready)
            done = ready
    for tiles in chunks:
        multiply(tiles, early, 2 * depth, False)
        for p in tiles:
            step_one(p)
    for p in range(parts):
        step_two(p)
    for p in range(parts):
        step_three(p)
    for p in range(parts):
        step_four(p)
    for p in range(parts):
        step_five(p)

    for n in range(pieces):
        pair[n].wait_send()
    for p in range(parts):
        for s in range(2):
            copy_one(p, s).wait_send()
            copy_two(p, s).wait_send()
        for d in range(SIDE):
            if d:
                copy_three(p, d).wait_send()
            for flip in range(2):
                if d or flip:
                    copy_four(p, d, flip).wait_send()


def solution(mesh):
    groups, members = mesh.shape["grp"], mesh.shape["mem"]

    def on_device(factors, screen):
        aux_rows, occ_count, basis = factors.shape
        depth = aux_rows * occ_count
        own = basis // (groups * members)
        parts = basis // 2 // LANES
        pieces = 4
        dma = pltpu.SemaphoreType.DMA
        vmem = pl.BlockSpec(memory_space=pltpu.VMEM)
        slots = 2 * SIDE - 1

        def codes(count, rows):
            return pltpu.VMEM((parts, count, rows, LANES), jnp.int16)

        return pl.pallas_call(
            functools.partial(kernel, members, occ_count // screen.shape[1], ORDERS, pieces),
            out_shape=jax.ShapeDtypeStruct((own, basis), jnp.float32),
            in_specs=[pl.BlockSpec(memory_space=pl.ANY), pl.BlockSpec(memory_space=pltpu.SMEM)],
            out_specs=vmem,
            scratch_shapes=[
                pltpu.VMEM((2 * depth, basis), jnp.bfloat16),
                pltpu.VMEM((basis, 2 * depth), jnp.bfloat16),
                pltpu.VMEM((parts, basis + 8, LANES), jnp.float32),
                pltpu.VMEM((parts, 512, LANES), jnp.float32),
                pltpu.VMEM((parts, 128, LANES), jnp.float32),
                codes(2, HEAD + 256), codes(2, HEAD + 256),
                codes(2, HEAD + 512), codes(2, HEAD + 512),
                codes(3, HEAD + 128), codes(3, HEAD + 128),
                codes(slots, 16), codes(slots, 16),
                dma((pieces,)), dma((pieces,)), dma((pieces,)),
                dma((parts, 2)), dma((parts, 2)),
                dma((parts, 2)), dma((parts, 2)),
                dma((parts, 3)), dma((parts, 3)),
                dma((parts, slots)), dma((parts, slots)),
            ],
            compiler_params=pltpu.CompilerParams(
                collective_id=0, has_side_effects=True, vmem_limit_bytes=60 * 1024 * 1024
            ),
        )(factors.reshape(depth, basis), screen)

    placed = (P(("grp", "mem"), None, None), P(("grp", "mem"), None))
    return jax.shard_map(
        on_device, mesh=mesh, in_specs=placed, out_specs=P(("grp", "mem"), None), check_vma=False
    )
```

```python
import functools

import jax
import jax.numpy as jnp
from jax import lax
from jax.experimental import pallas as pl
from jax.experimental.pallas import tpu as pltpu
from jax.sharding import PartitionSpec as P

LANES = 128
TOP = 32767.0
SIDE = 4
HEAD = 16
MESH = pl.DeviceIdType.MESH
ORDERS = ("yzx", "zxy", "xyz", "yzx", "zxy", "xyz", "wvz")
PIECES = (192, 256, 128)


def kernel(
    members, width, orders, pieces,
    x_ref, screen_ref, out_ref,
    both, turned, total, first_sum, second_sum,
    out_one, in_one, out_two, in_two, out_three, in_three, out_four, in_four,
    load_sem, pair_send, pair_recv, one_send, one_recv, two_send, two_recv,
    three_send, three_recv, four_send, four_recv,
):
    depth, basis = x_ref.shape
    own = out_ref.shape[0]
    half = basis // 2
    parts = len(orders)
    occ_blocks = screen_ref.shape[1]
    grp, mem = lax.axis_index("grp"), lax.axis_index("mem")
    at = {"y": lax.div(grp, 2), "c": lax.rem(grp, 2), "x": lax.div(mem, SIDE), "z": lax.rem(mem, SIDE)}
    core = at["c"]

    at["w"] = (1 - core) * at["y"] + core * at["x"]
    at["v"] = core * at["y"] + (1 - core) * at["x"]

    def place(axis, d):
        return lax.rem(at[axis] + d, SIDE)

    def device(axis, d, flip=0):
        there = dict(at)
        if d and axis in "wv":
            moved = place(axis, d)
            on_y = 1 - core if axis == "w" else core
            there["y"] = on_y * moved + (1 - on_y) * at["y"]
            there["x"] = (1 - on_y) * moved + on_y * at["x"]
        elif d:
            there[axis] = place(axis, d)
        if flip:
            there["c"] = 1 - core
        return (there["y"] * 2 + there["c"], there["x"] * SIDE + there["z"])

    last_axes = sorted({order[2] for order in orders})
    peers = [device("x", 0, 1)]
    for axis in "xyz":
        for d in range(1, SIDE):
            peers.append(device(axis, d))
            if axis in last_axes:
                peers.append(device(axis, d, 1))
    barrier = pltpu.get_barrier_semaphore()
    for other in peers:
        pl.semaphore_signal(barrier, inc=1, device_id=other, device_id_type=MESH)

    starts = [sum(pieces[:n]) for n in range(len(pieces) + 1)]
    loads = []
    for n in range(len(pieces)):
        rows = pl.ds(starts[n], pieces[n])
        loads.append(pltpu.make_async_copy(x_ref.at[rows], both.at[rows], load_sem.at[n]))
        loads[-1].start()

    total_rows = total.shape[1]
    for p in range(parts):
        total[p, basis:total_rows, :] = jnp.zeros((total_rows - basis, LANES), jnp.float32)
        tail = second_sum.shape[1]
        second_sum[p, tail - 16 : tail, :] = jnp.zeros((16, LANES), jnp.float32)
        first_sum[p, 448:464, :] = jnp.zeros((16, LANES), jnp.float32)

    def mask(j, carry):
        rows = pl.ds(pl.multiple_of(j * width, width), width)
        keep = screen_ref[0, lax.rem(j, occ_blocks)].astype(jnp.float32)
        both[rows, :] = (both[rows, :].astype(jnp.float32) * keep).astype(both.dtype)
        return carry

    pair = []
    partner = device("x", 0, 1)
    for n in range(len(pieces)):
        loads[n].wait()
        lax.fori_loop(starts[n] // width, starts[n + 1] // width, mask, 0)
        if n == 0:
            pl.semaphore_wait(barrier, len(peers))
        pair.append(
            pltpu.make_async_remote_copy(
                src_ref=both.at[pl.ds(starts[n], pieces[n])],
                dst_ref=both.at[pl.ds(depth + starts[n], pieces[n])],
                send_sem=pair_send.at[n], recv_sem=pair_recv.at[n],
                device_id=partner, device_id_type=MESH,
            )
        )
        pair[-1].start()

    def turn(low, high):
        def one(m, carry):
            rows = pl.ds(pl.multiple_of(m * 256, 256), 256)
            for k in range(low, high, LANES):
                turned[rows, k : k + LANES] = both[k : k + LANES, rows].T
            return carry

        lax.fori_loop(0, basis // 256, one, 0)

    def multiply(tiles, low, high, fresh):
        tall = basis // 2
        columns = pl.ds(pl.multiple_of(core * half + tiles[0] * LANES, LANES), len(tiles) * LANES)

        def one(m, carry):
            rows = pl.ds(pl.multiple_of(m * tall, LANES), tall)
            value = jnp.dot(turned[rows, low:high], both[low:high, columns], preferred_element_type=jnp.float32)
            for n, p in enumerate(tiles):
                mine = value[:, n * LANES : (n + 1) * LANES]
                total[p, rows, :] = mine if fresh else total[p, rows, :] + mine
            return carry

        lax.fori_loop(0, 2, one, 0)

    def exponent(top):
        return jnp.floor(jnp.log(jnp.maximum(top, 1e-33)) * 1.4426950408889634) + 1.0

    def coded(value, power):
        return jnp.round(value * (jnp.exp2(-power) * TOP)).astype(jnp.int32).astype(jnp.int16)

    def put(ref, values):
        rows = lax.broadcasted_iota(jnp.int32, (HEAD, LANES), 0)
        head = jnp.zeros((HEAD, LANES), jnp.float32)
        for g, value in enumerate(values):
            power = exponent(jnp.max(jnp.abs(value), axis=0, keepdims=True))
            n = value.shape[0]
            ref[HEAD + g * n : HEAD + (g + 1) * n, :] = coded(value, power)
            head = jnp.where(rows == g, power, head)
        ref[0:HEAD, :] = head.astype(jnp.int32).astype(jnp.int16)

    def powers(ref):
        return jnp.exp2(ref[0:HEAD, :].astype(jnp.int32).astype(jnp.float32)) * (1.0 / TOP)

    def get(ref, scale, g, n):
        return ref[HEAD + g * n : HEAD + (g + 1) * n, :].astype(jnp.int32).astype(jnp.float32) * scale[g : g + 1, :]

    def group_rows(order):
        return 128 if order[0] == "z" else 112

    def load(p, order, block, c, g):
        if order[0] == "y":
            start = block * (8 * own * SIDE) + c * (4 * own * SIDE) + g * 112
            return total[p, pl.ds(pl.multiple_of(start, 8), 112), :]
        if order[0] in "xw":
            near, far = own * SIDE, 8 * own * SIDE
            if order[0] == "w":
                near, far = core * near + (1 - core) * far, (1 - core) * near + core * far
            starts = [(2 * g + n) * far + c * (4 * own * SIDE) + block * near for n in range(2)]
            return jnp.concatenate([total[p, pl.ds(pl.multiple_of(s, 8), 56), :] for s in starts], axis=0)
        starts = [
            (2 * g + n) * (8 * own * SIDE) + c * (4 * own * SIDE) + m * (own * SIDE) + block * own
            for n in range(2) for m in range(SIDE)
        ]
        return jnp.concatenate([total[p, pl.ds(s, 16), :] for s in starts], axis=0)

    def second_block(p, order, j):
        if order[1] == "z":
            starts = [c * (4 * own * SIDE) + m * (own * SIDE) + j * own for c in range(2) for m in range(SIDE)]
            return jnp.concatenate([first_sum[p, pl.ds(s, 16), :] for s in starts], axis=0)
        if order[0] != "z" or order[1] == "y":
            n = 64 if order[0] == "z" else 56
            starts = [c * 4 * n + j * n for c in range(2)]
        else:
            n = 16
            starts = [c * 256 + m * 64 + j * n for c in range(2) for m in range(SIDE)]
        return jnp.concatenate([first_sum[p, pl.ds(pl.multiple_of(s, 8), n), :] for s in starts], axis=0)

    def copy(here, there, a, b, to):
        return pltpu.make_async_remote_copy(
            src_ref=here, dst_ref=there, send_sem=a, recv_sem=b, device_id=to, device_id_type=MESH,
        )

    def sized(order, groups):
        return pl.ds(0, HEAD + groups * group_rows(order))

    def copy_one(p, s):
        order = orders[p]
        run = sized(order, 2)
        return copy(out_one.at[p, s, run], in_one.at[p, s, run], one_send.at[p, s], one_recv.at[p, s],
                    device(order[0], (1, 3)[s]))

    def copy_two(p, s):
        order = orders[p]
        run = sized(order, 4)
        return copy(out_two.at[p, s, run], in_two.at[p, s, run], two_send.at[p, s], two_recv.at[p, s],
                    device(order[0], (1, 3)[s]))

    def second_rows(order):
        return 128 if "z" in order[:2] else 112

    def copy_three(p, d):
        order = orders[p]
        run = pl.ds(0, HEAD + second_rows(order))
        return copy(out_three.at[p, d - 1, run], in_three.at[p, d - 1, run], three_send.at[p, d - 1],
                    three_recv.at[p, d - 1], device(order[1], d))

    def copy_four(p, d, flip):
        s = 2 * d + flip - 1
        return copy(out_four.at[p, s], in_four.at[p, s], four_send.at[p, s], four_recv.at[p, s],
                    device(orders[p][2], d, flip))

    def step_one(p):
        order = orders[p]
        block = place(order[0], 2)
        for s in range(2):
            put(out_one.at[p, s], [load(p, order, block, s, g) for g in range(2)])
            copy_one(p, s).start()

    def step_two(p):
        order = orders[p]
        n = group_rows(order)
        for s in range(2):
            copy_one(p, s).wait_recv()
            block = place(order[0], (1, 3)[s])
            scale = powers(in_one.at[p, s])
            values = []
            for c in range(2):
                for g in range(2):
                    value = load(p, order, block, c, g)
                    if c == s:
                        value = value + get(in_one.at[p, s], scale, g, n)
                    values.append(value)
            put(out_two.at[p, s], values)
            copy_two(p, s).start()

    def step_three(p):
        order = orders[p]
        n = group_rows(order)
        for s in range(2):
            copy_two(p, s).wait_recv()
        scales = [powers(in_two.at[p, s]) for s in range(2)]
        for c in range(2):
            for g in range(2):
                value = load(p, order, at[order[0]], c, g)
                for s in range(2):
                    value = value + get(in_two.at[p, s], scales[s], 2 * c + g, n)
                first_sum[p, (2 * c + g) * n : (2 * c + g + 1) * n, :] = value
        for d in range(1, SIDE):
            put(out_three.at[p, d - 1], [second_block(p, order, place(order[1], d))])
            copy_three(p, d).start()

    def last_rows(order, c, k):
        if "z" in order[:2]:
            return pl.ds(pl.multiple_of(c * 64 + k * 16, 8), 16)
        return pl.ds(c * 4 * own + k * own, 16)

    def step_four(p):
        order = orders[p]
        n = second_rows(order)
        value = second_block(p, order, at[order[1]])
        for d in range(1, SIDE):
            copy_three(p, d).wait_recv()
            ref = in_three.at[p, d - 1]
            value = value + get(ref, powers(ref), 0, n)
        second_sum[p, 0:n, :] = value
        rows = lax.broadcasted_iota(jnp.int32, (16, LANES), 0)
        for d in range(SIDE):
            for flip in range(2):
                if d or flip:
                    c = 1 - core if flip else core
                    value = second_sum[p, last_rows(order, c, place(order[2], d)), :]
                    top = jnp.max(jnp.where(rows < own, jnp.abs(value), 0.0), axis=0, keepdims=True)
                    power = exponent(top)
                    code = jnp.round(value * (jnp.exp2(-power) * TOP))
                    code = jnp.where(rows < own, code, power)
                    out_four[p, 2 * d + flip - 1] = code.astype(jnp.int32).astype(jnp.int16)
                    copy_four(p, d, flip).start()

    def step_five(p):
        order = orders[p]
        for flip in range(2):
            c = 1 - core if flip else core
            value = None
            if not flip:
                value = second_sum[p, last_rows(order, core, at[order[2]]), :]
            for d in range(SIDE):
                if d or flip:
                    copy_four(p, d, flip).wait_recv()
                    code = in_four[p, 2 * d + flip - 1].astype(jnp.int32).astype(jnp.float32)
                    term = code * (jnp.exp2(code[own : own + 1, :]) * (1.0 / TOP))
                    value = term if value is None else value + term
            columns = pl.ds(pl.multiple_of(c * half + p * LANES, LANES), LANES)
            out_ref[:, columns] = value[0:own, :]

    first, rest = [0, 1, 2], [[3, 4], [5, 6]]
    edges = [depth // LANES * LANES] + [depth + start for start in starts[1:]]
    turn(0, edges[0])
    multiply(first, 0, edges[0], True)
    for n in range(len(pieces)):
        pair[n].wait_recv()
        turn(edges[n], edges[n + 1])
        multiply(first, edges[n], edges[n + 1], False)
    for p in first:
        step_one(p)
    for tiles in rest:
        multiply(tiles, 0, 2 * depth, True)
        for p in tiles:
            step_one(p)
    for p in range(parts):
        step_two(p)
    for p in range(parts):
        step_three(p)
    for p in range(parts):
        step_four(p)
    for p in range(parts):
        step_five(p)

    for n in range(len(pieces)):
        pair[n].wait_send()
    for p in range(parts):
        for s in range(2):
            copy_one(p, s).wait_send()
            copy_two(p, s).wait_send()
        for d in range(SIDE):
            if d:
                copy_three(p, d).wait_send()
            for flip in range(2):
                if d or flip:
                    copy_four(p, d, flip).wait_send()


def solution(mesh):
    groups, members = mesh.shape["grp"], mesh.shape["mem"]

    def on_device(factors, screen):
        aux_rows, occ_count, basis = factors.shape
        depth = aux_rows * occ_count
        own = basis // (groups * members)
        parts = basis // 2 // LANES
        pieces = PIECES
        dma = pltpu.SemaphoreType.DMA
        vmem = pl.BlockSpec(memory_space=pltpu.VMEM)
        slots = 2 * SIDE - 1

        def codes(count, rows):
            return pltpu.VMEM((parts, count, rows, LANES), jnp.int16)

        return pl.pallas_call(
            functools.partial(kernel, members, occ_count // screen.shape[1], ORDERS, pieces),
            out_shape=jax.ShapeDtypeStruct((own, basis), jnp.float32),
            in_specs=[pl.BlockSpec(memory_space=pl.ANY), pl.BlockSpec(memory_space=pltpu.SMEM)],
            out_specs=vmem,
            scratch_shapes=[
                pltpu.VMEM((2 * depth, basis), jnp.bfloat16),
                pltpu.VMEM((basis, 2 * depth), jnp.bfloat16),
                pltpu.VMEM((parts, basis + 8, LANES), jnp.float32),
                pltpu.VMEM((parts, 512, LANES), jnp.float32),
                pltpu.VMEM((parts, 128, LANES), jnp.float32),
                codes(2, HEAD + 256), codes(2, HEAD + 256),
                codes(2, HEAD + 512), codes(2, HEAD + 512),
                codes(3, HEAD + 128), codes(3, HEAD + 128),
                codes(slots, 16), codes(slots, 16),
                dma((len(pieces),)), dma((len(pieces),)), dma((len(pieces),)),
                dma((parts, 2)), dma((parts, 2)),
                dma((parts, 2)), dma((parts, 2)),
                dma((parts, 3)), dma((parts, 3)),
                dma((parts, slots)), dma((parts, slots)),
            ],
            compiler_params=pltpu.CompilerParams(
                collective_id=0, has_side_effects=True, vmem_limit_bytes=60 * 1024 * 1024
            ),
        )(factors.reshape(depth, basis), screen)

    placed = (P(("grp", "mem"), None, None), P(("grp", "mem"), None))
    return jax.shard_map(
        on_device, mesh=mesh, in_specs=placed, out_specs=P(("grp", "mem"), None), check_vma=False
    )
```

```python
import functools

import jax
import jax.numpy as jnp
from jax import lax
from jax.experimental import pallas as pl
from jax.experimental.pallas import tpu as pltpu
from jax.sharding import PartitionSpec as P

LANES = 128
TOP = 32767.0
SIDE = 4
HEAD = 16
MESH = pl.DeviceIdType.MESH
ORDERS = ("yzx", "zxy", "xyz", "yzx", "zxy", "xyz", "wvz")
PIECES = (192, 256, 128)
MERGED = (3, 4, 5, 6)
PLANE = 2 * SIDE * SIDE - 1


def kernel(
    members, width, orders, pieces,
    x_ref, flags_ref, out_ref,
    screen_ref, both, turned, total, first_sum, second_sum,
    out_one, in_one, out_two, in_two, out_three, in_three, out_four, in_four, out_plane, in_plane,
    flag_sem, load_sem, pair_send, pair_recv, one_send, one_recv, two_send, two_recv,
    three_send, three_recv, four_send, four_recv, plane_send, plane_recv,
):
    depth, basis = x_ref.shape
    own = out_ref.shape[0]
    half = basis // 2
    parts = len(orders)
    occ_blocks = screen_ref.shape[1]
    grp, mem = lax.axis_index("grp"), lax.axis_index("mem")
    at = {"y": lax.div(grp, 2), "c": lax.rem(grp, 2), "x": lax.div(mem, SIDE), "z": lax.rem(mem, SIDE)}
    core = at["c"]

    at["w"] = (1 - core) * at["y"] + core * at["x"]
    at["v"] = core * at["y"] + (1 - core) * at["x"]

    def place(axis, d):
        return lax.rem(at[axis] + d, SIDE)

    def device(axis, d, flip=0):
        return moved([(axis, d)], flip)

    def moved(moves, flip=0):
        there = dict(at)
        for axis, d in moves:
            if d and axis in "wv":
                to = place(axis, d)
                on_y = 1 - core if axis == "w" else core
                there["y"] = on_y * to + (1 - on_y) * there["y"]
                there["x"] = (1 - on_y) * to + on_y * there["x"]
            elif d:
                there[axis] = place(axis, d)
        if flip:
            there["c"] = 1 - core
        return (there["y"] * 2 + there["c"], there["x"] * SIDE + there["z"])

    last_axes = sorted({order[2] for order in orders})
    peers = [device("x", 0, 1)]
    for axis in "xyz":
        for d in range(1, SIDE):
            peers.append(device(axis, d))
            if axis in last_axes:
                peers.append(device(axis, d, 1))
    barrier = pltpu.get_barrier_semaphore()
    for other in peers:
        pl.semaphore_signal(barrier, inc=1, device_id=other, device_id_type=MESH)

    starts = [sum(pieces[:n]) for n in range(len(pieces) + 1)]
    flags = pltpu.make_async_copy(flags_ref, screen_ref, flag_sem)
    flags.start()
    loads = []
    for n in range(len(pieces)):
        rows = pl.ds(starts[n], pieces[n])
        loads.append(pltpu.make_async_copy(x_ref.at[rows], both.at[rows], load_sem.at[n]))
        loads[-1].start()

    total_rows = total.shape[1]
    for p in range(parts):
        total[p, basis:total_rows, :] = jnp.zeros((total_rows - basis, LANES), jnp.float32)
        tail = second_sum.shape[1]
        second_sum[p, tail - 16 : tail, :] = jnp.zeros((16, LANES), jnp.float32)
        first_sum[p, 448:464, :] = jnp.zeros((16, LANES), jnp.float32)

    def mask(j, carry):
        rows = pl.ds(pl.multiple_of(j * width, width), width)
        keep = screen_ref[0, lax.rem(j, occ_blocks)].astype(jnp.float32)
        both[rows, :] = (both[rows, :].astype(jnp.float32) * keep).astype(both.dtype)
        return carry

    pair = []
    partner = device("x", 0, 1)
    flags.wait()
    for n in range(len(pieces)):
        loads[n].wait()
        lax.fori_loop(starts[n] // width, starts[n + 1] // width, mask, 0)
        if n == 0:
            pl.semaphore_wait(barrier, len(peers))
        pair.append(
            pltpu.make_async_remote_copy(
                src_ref=both.at[pl.ds(starts[n], pieces[n])],
                dst_ref=both.at[pl.ds(depth + starts[n], pieces[n])],
                send_sem=pair_send.at[n], recv_sem=pair_recv.at[n],
                device_id=partner, device_id_type=MESH,
            )
        )
        pair[-1].start()

    def turn(low, high):
        def one(m, carry):
            rows = pl.ds(pl.multiple_of(m * 256, 256), 256)
            for k in range(low, high, LANES):
                turned[rows, k : k + LANES] = both[k : k + LANES, rows].T
            return carry

        lax.fori_loop(0, basis // 256, one, 0)

    def multiply(tiles, low, high, fresh):
        tall = basis // 2
        columns = pl.ds(pl.multiple_of(core * half + tiles[0] * LANES, LANES), len(tiles) * LANES)

        def one(m, carry):
            rows = pl.ds(pl.multiple_of(m * tall, LANES), tall)
            value = jnp.dot(turned[rows, low:high], both[low:high, columns], preferred_element_type=jnp.float32)
            for n, p in enumerate(tiles):
                mine = value[:, n * LANES : (n + 1) * LANES]
                total[p, rows, :] = mine if fresh else total[p, rows, :] + mine
            return carry

        lax.fori_loop(0, 2, one, 0)

    def exponent(top):
        return jnp.floor(jnp.log(jnp.maximum(top, 1e-33)) * 1.4426950408889634) + 1.0

    def coded(value, power):
        return jnp.round(value * (jnp.exp2(-power) * TOP)).astype(jnp.int32).astype(jnp.int16)

    def put(ref, values):
        rows = lax.broadcasted_iota(jnp.int32, (HEAD, LANES), 0)
        head = jnp.zeros((HEAD, LANES), jnp.float32)
        for g, value in enumerate(values):
            power = exponent(jnp.max(jnp.abs(value), axis=0, keepdims=True))
            n = value.shape[0]
            ref[HEAD + g * n : HEAD + (g + 1) * n, :] = coded(value, power)
            head = jnp.where(rows == g, power, head)
        ref[0:HEAD, :] = head.astype(jnp.int32).astype(jnp.int16)

    def powers(ref):
        return jnp.exp2(ref[0:HEAD, :].astype(jnp.int32).astype(jnp.float32)) * (1.0 / TOP)

    def get(ref, scale, g, n):
        return ref[HEAD + g * n : HEAD + (g + 1) * n, :].astype(jnp.int32).astype(jnp.float32) * scale[g : g + 1, :]

    def group_rows(order):
        return 128 if order[0] == "z" else 112

    def load(p, order, block, c, g):
        if order[0] == "y":
            start = block * (8 * own * SIDE) + c * (4 * own * SIDE) + g * 112
            return total[p, pl.ds(pl.multiple_of(start, 8), 112), :]
        if order[0] in "xw":
            near, far = own * SIDE, 8 * own * SIDE
            if order[0] == "w":
                near, far = core * near + (1 - core) * far, (1 - core) * near + core * far
            starts = [(2 * g + n) * far + c * (4 * own * SIDE) + block * near for n in range(2)]
            return jnp.concatenate([total[p, pl.ds(pl.multiple_of(s, 8), 56), :] for s in starts], axis=0)
        starts = [
            (2 * g + n) * (8 * own * SIDE) + c * (4 * own * SIDE) + m * (own * SIDE) + block * own
            for n in range(2) for m in range(SIDE)
        ]
        return jnp.concatenate([total[p, pl.ds(s, 16), :] for s in starts], axis=0)

    def second_block(p, order, j):
        if order[1] == "z":
            starts = [c * (4 * own * SIDE) + m * (own * SIDE) + j * own for c in range(2) for m in range(SIDE)]
            return jnp.concatenate([first_sum[p, pl.ds(s, 16), :] for s in starts], axis=0)
        if order[0] != "z" or order[1] == "y":
            n = 64 if order[0] == "z" else 56
            starts = [c * 4 * n + j * n for c in range(2)]
        else:
            n = 16
            starts = [c * 256 + m * 64 + j * n for c in range(2) for m in range(SIDE)]
        return jnp.concatenate([first_sum[p, pl.ds(pl.multiple_of(s, 8), n), :] for s in starts], axis=0)

    def copy(here, there, a, b, to):
        return pltpu.make_async_remote_copy(
            src_ref=here, dst_ref=there, send_sem=a, recv_sem=b, device_id=to, device_id_type=MESH,
        )

    def sized(order, groups):
        return pl.ds(0, HEAD + groups * group_rows(order))

    def copy_one(p, s):
        order = orders[p]
        run = sized(order, 2)
        return copy(out_one.at[p, s, run], in_one.at[p, s, run], one_send.at[p, s], one_recv.at[p, s],
                    device(order[0], (1, 3)[s]))

    def copy_two(p, s, late):
        order = orders[p]
        run = sized(order, 2)
        n = 2 * s + late
        return copy(out_two.at[p, n, run], in_two.at[p, n, run], two_send.at[p, n], two_recv.at[p, n],
                    device(order[0], (1, 3)[s]))

    def second_rows(order):
        return 128 if "z" in order[:2] else 112

    def copy_three(p, d):
        order = orders[p]
        run = pl.ds(0, HEAD + second_rows(order))
        return copy(out_three.at[p, d - 1, run], in_three.at[p, d - 1, run], three_send.at[p, d - 1],
                    three_recv.at[p, d - 1], device(order[1], d))

    def copy_four(p, d, flip):
        s = 2 * d + flip - 1
        return copy(out_four.at[p, s], in_four.at[p, s], four_send.at[p, s], four_recv.at[p, s],
                    device(orders[p][2], d, flip))

    def step_one(p):
        order = orders[p]
        block = place(order[0], 2)
        for s in range(2):
            put(out_one.at[p, s], [load(p, order, block, s, g) for g in range(2)])
            copy_one(p, s).start()

    def step_solo(p):
        order = orders[p]
        for s in range(2):
            block = place(order[0], (1, 3)[s])
            put(out_two.at[p, 2 * s], [load(p, order, block, 1 - s, g) for g in range(2)])
            copy_two(p, s, 0).start()

    def step_two(p):
        order = orders[p]
        n = group_rows(order)
        for s in range(2):
            copy_one(p, s).wait_recv()
            block = place(order[0], (1, 3)[s])
            ref = in_one.at[p, s]
            scale = powers(ref)
            put(out_two.at[p, 2 * s + 1], [load(p, order, block, s, g) + get(ref, scale, g, n) for g in range(2)])
            copy_two(p, s, 1).start()

    def collect(p):
        order = orders[p]
        n = group_rows(order)
        for s in range(2):
            for late in range(2):
                copy_two(p, s, late).wait_recv()
        for c in range(2):
            refs = [in_two.at[p, 2 * s + (1 if c == s else 0)] for s in range(2)]
            scales = [powers(ref) for ref in refs]
            for g in range(2):
                value = load(p, order, at[order[0]], c, g)
                for ref, scale in zip(refs, scales):
                    value = value + get(ref, scale, g, n)
                first_sum[p, (2 * c + g) * n : (2 * c + g + 1) * n, :] = value

    def plane_rows(order, c, u, v):
        if order[0] == "z":
            steps = {"y": SIDE * 16, "x": 16} if order[1] == "y" else {"x": 16, "y": SIDE * 16}
            return pl.ds(pl.multiple_of(c * 256 + u * steps[order[1]] + v * steps[order[2]], 8), 16)
        step = own if order[1] == "z" else own * SIDE
        other = own * SIDE if order[1] == "z" else own
        return pl.ds(c * (4 * own * SIDE) + u * step + v * other, 16)

    def plane_slot(du, dv, flip):
        return (du * SIDE + dv) * 2 + flip - 1

    def step_plane(q):
        p = merged[q]
        order = orders[p]
        collect(p)
        row = lax.rem(lax.broadcasted_iota(jnp.int32, (SIDE * 16, LANES), 0), 16)
        for du in range(SIDE):
            u = place(order[1], du)
            for flip in range(2):
                c = 1 - core if flip else core
                value = jnp.concatenate(
                    [first_sum[p, plane_rows(order, c, u, place(order[2], dv)), :] for dv in range(SIDE)], axis=0
                )
                power = exponent(jnp.max(jnp.abs(value), axis=0, keepdims=True))
                code = jnp.where(row == own, power, jnp.round(value * (jnp.exp2(-power) * TOP)))
                code = code.astype(jnp.int32).astype(jnp.int16)
                for dv in range(SIDE):
                    if du or dv or flip:
                        n = plane_slot(du, dv, flip)
                        out_plane[q, n] = code[dv * 16 : (dv + 1) * 16, :]
                        copy(out_plane.at[q, n], in_plane.at[q, n], plane_send.at[q], plane_recv.at[q],
                             moved([(order[1], du), (order[2], dv)], flip)).start()

    def wait_plane(q, sent):
        whole = copy(out_plane.at[q], in_plane.at[q], plane_send.at[q], plane_recv.at[q], partner)
        whole.wait_send() if sent else whole.wait_recv()

    def end_plane(q):
        p = merged[q]
        order = orders[p]
        wait_plane(q, False)
        for flip in range(2):
            c = 1 - core if flip else core
            value = None
            if not flip:
                value = first_sum[p, plane_rows(order, core, at[order[1]], at[order[2]]), :]
            for du in range(SIDE):
                for dv in range(SIDE):
                    if du or dv or flip:
                        code = in_plane[q, plane_slot(du, dv, flip)].astype(jnp.int32).astype(jnp.float32)
                        term = code * (jnp.exp2(code[own : own + 1, :]) * (1.0 / TOP))
                        value = term if value is None else value + term
            columns = pl.ds(pl.multiple_of(c * half + p * LANES, LANES), LANES)
            out_ref[:, columns] = value[0:own, :]

    def step_three(p):
        order = orders[p]
        collect(p)
        for d in range(1, SIDE):
            put(out_three.at[p, d - 1], [second_block(p, order, place(order[1], d))])
            copy_three(p, d).start()

    def last_rows(order, c, k):
        if "z" in order[:2]:
            return pl.ds(pl.multiple_of(c * 64 + k * 16, 8), 16)
        return pl.ds(c * 4 * own + k * own, 16)

    def step_four(p):
        order = orders[p]
        n = second_rows(order)
        value = second_block(p, order, at[order[1]])
        for d in range(1, SIDE):
            copy_three(p, d).wait_recv()
            ref = in_three.at[p, d - 1]
            value = value + get(ref, powers(ref), 0, n)
        second_sum[p, 0:n, :] = value
        rows = lax.broadcasted_iota(jnp.int32, (16, LANES), 0)
        for d in range(SIDE):
            for flip in range(2):
                if d or flip:
                    c = 1 - core if flip else core
                    value = second_sum[p, last_rows(order, c, place(order[2], d)), :]
                    top = jnp.max(jnp.where(rows < own, jnp.abs(value), 0.0), axis=0, keepdims=True)
                    power = exponent(top)
                    code = jnp.round(value * (jnp.exp2(-power) * TOP))
                    code = jnp.where(rows < own, code, power)
                    out_four[p, 2 * d + flip - 1] = code.astype(jnp.int32).astype(jnp.int16)
                    copy_four(p, d, flip).start()

    def step_five(p):
        order = orders[p]
        for flip in range(2):
            c = 1 - core if flip else core
            value = None
            if not flip:
                value = second_sum[p, last_rows(order, core, at[order[2]]), :]
            for d in range(SIDE):
                if d or flip:
                    copy_four(p, d, flip).wait_recv()
                    code = in_four[p, 2 * d + flip - 1].astype(jnp.int32).astype(jnp.float32)
                    term = code * (jnp.exp2(code[own : own + 1, :]) * (1.0 / TOP))
                    value = term if value is None else value + term
            columns = pl.ds(pl.multiple_of(c * half + p * LANES, LANES), LANES)
            out_ref[:, columns] = value[0:own, :]

    first, rest = [0, 1, 2], [[3, 4, 5, 6]]
    merged = MERGED
    apart = [p for p in range(parts) if p not in merged]
    edges = [depth // LANES * LANES] + [depth + start for start in starts[1:]]
    turn(0, edges[0])
    multiply(first, 0, edges[0], True)
    for n in range(len(pieces)):
        pair[n].wait_recv()
        turn(edges[n], edges[n + 1])
        multiply(first, edges[n], edges[n + 1], False)
    for p in first:
        step_one(p)
    for p in first:
        step_solo(p)
    late = rest[0]
    multiply(late, 0, 2 * depth, True)
    for p in late:
        step_one(p)
    for p in first:
        step_two(p)
    for p in late:
        step_solo(p)
    for p in late:
        step_two(p)
    for p in first:
        step_plane(merged.index(p)) if p in merged else step_three(p)
    for p in late:
        step_plane(merged.index(p)) if p in merged else step_three(p)
    for p in apart:
        step_four(p)
    for q in range(len(merged)):
        end_plane(q)
    for p in apart:
        step_five(p)

    for n in range(len(pieces)):
        pair[n].wait_send()
    for p in range(parts):
        for s in range(2):
            copy_one(p, s).wait_send()
            for late in range(2):
                copy_two(p, s, late).wait_send()
    for q in range(len(merged)):
        wait_plane(q, True)
    for p in apart:
        for d in range(SIDE):
            if d:
                copy_three(p, d).wait_send()
            for flip in range(2):
                if d or flip:
                    copy_four(p, d, flip).wait_send()


def solution(mesh):
    groups, members = mesh.shape["grp"], mesh.shape["mem"]

    def on_device(factors, screen):
        aux_rows, occ_count, basis = factors.shape
        depth = aux_rows * occ_count
        own = basis // (groups * members)
        parts = basis // 2 // LANES
        pieces = PIECES
        dma = pltpu.SemaphoreType.DMA
        vmem = pl.BlockSpec(memory_space=pltpu.VMEM)
        slots = 2 * SIDE - 1

        def codes(count, rows):
            return pltpu.VMEM((parts, count, rows, LANES), jnp.int16)

        return pl.pallas_call(
            functools.partial(kernel, members, occ_count // screen.shape[1], ORDERS, pieces),
            out_shape=jax.ShapeDtypeStruct((own, basis), jnp.float32),
            in_specs=[pl.BlockSpec(memory_space=pltpu.HBM)] * 2,
            out_specs=vmem,
            scratch_shapes=[
                pltpu.SMEM(screen.shape, jnp.int32),
                pltpu.VMEM((2 * depth, basis), jnp.bfloat16),
                pltpu.VMEM((basis, 2 * depth), jnp.bfloat16),
                pltpu.VMEM((parts, basis + 8, LANES), jnp.float32),
                pltpu.VMEM((parts, 512, LANES), jnp.float32),
                pltpu.VMEM((parts, 128, LANES), jnp.float32),
                codes(2, HEAD + 256), codes(2, HEAD + 256),
                codes(4, HEAD + 256), codes(4, HEAD + 256),
                codes(3, HEAD + 128), codes(3, HEAD + 128),
                codes(slots, 16), codes(slots, 16),
                pltpu.VMEM((len(MERGED), PLANE, 16, LANES), jnp.int16),
                pltpu.VMEM((len(MERGED), PLANE, 16, LANES), jnp.int16),
                dma, dma((len(pieces),)), dma((len(pieces),)), dma((len(pieces),)),
                dma((parts, 2)), dma((parts, 2)),
                dma((parts, 4)), dma((parts, 4)),
                dma((parts, 3)), dma((parts, 3)),
                dma((parts, slots)), dma((parts, slots)),
                dma((len(MERGED),)), dma((len(MERGED),)),
            ],
            compiler_params=pltpu.CompilerParams(
                collective_id=0, has_side_effects=True, vmem_limit_bytes=53 * 1024 * 1024
            ),
        )(factors.reshape(depth, basis), screen)

    placed = (P(("grp", "mem"), None, None), P(("grp", "mem"), None))
    return jax.shard_map(
        on_device, mesh=mesh, in_specs=placed, out_specs=P(("grp", "mem"), None), check_vma=False
    )
```

```python
import functools

import jax
import jax.numpy as jnp
from jax import lax
from jax.experimental import pallas as pl
from jax.experimental.pallas import tpu as pltpu
from jax.sharding import PartitionSpec as P

LANES = 128
TOP = 32767.0
SIDE = 4
HEAD = 16
MESH = pl.DeviceIdType.MESH
ORDERS = ("yzx", "zxy", "xyz", "yzx", "zxy", "xyz", "wvz")
PIECES = (192, 256, 128)
MERGED = (3, 4, 5, 6)
PLANE = 2 * SIDE * SIDE - 1


def kernel(
    members, width, orders, pieces,
    x_ref, flags_ref, out_ref,
    screen_ref, both, turned, total, first_sum, second_sum,
    out_one, in_one, out_two, in_two, out_three, in_three, out_four, in_four, out_plane, in_plane,
    flag_sem, load_sem, pair_send, pair_recv, one_send, one_recv, two_send, two_recv,
    three_send, three_recv, four_send, four_recv, plane_send, plane_recv,
):
    depth, basis = x_ref.shape
    own = out_ref.shape[0]
    half = basis // 2
    parts = len(orders)
    occ_blocks = screen_ref.shape[1]
    grp, mem = lax.axis_index("grp"), lax.axis_index("mem")
    at = {"y": lax.div(grp, 2), "c": lax.rem(grp, 2), "x": lax.div(mem, SIDE), "z": lax.rem(mem, SIDE)}
    core = at["c"]

    at["w"] = (1 - core) * at["y"] + core * at["x"]
    at["v"] = core * at["y"] + (1 - core) * at["x"]

    def place(axis, d):
        return lax.rem(at[axis] + d, SIDE)

    def device(axis, d, flip=0):
        return moved([(axis, d)], flip)

    def moved(moves, flip=0):
        there = dict(at)
        for axis, d in moves:
            if d and axis in "wv":
                to = place(axis, d)
                on_y = 1 - core if axis == "w" else core
                there["y"] = on_y * to + (1 - on_y) * there["y"]
                there["x"] = (1 - on_y) * to + on_y * there["x"]
            elif d:
                there[axis] = place(axis, d)
        if flip:
            there["c"] = 1 - core
        return (there["y"] * 2 + there["c"], there["x"] * SIDE + there["z"])

    last_axes = sorted({order[2] for order in orders})
    peers = [device("x", 0, 1)]
    for axis in "xyz":
        for d in range(1, SIDE):
            peers.append(device(axis, d))
            if axis in last_axes:
                peers.append(device(axis, d, 1))
    barrier = pltpu.get_barrier_semaphore()
    for other in peers:
        pl.semaphore_signal(barrier, inc=1, device_id=other, device_id_type=MESH)

    starts = [sum(pieces[:n]) for n in range(len(pieces) + 1)]
    flags = pltpu.make_async_copy(flags_ref, screen_ref, flag_sem)
    flags.start()
    loads = []
    for n in range(len(pieces)):
        rows = pl.ds(starts[n], pieces[n])
        loads.append(pltpu.make_async_copy(x_ref.at[rows], both.at[rows], load_sem.at[n]))
        loads[-1].start()

    total_rows = total.shape[1]
    for p in range(parts):
        total[p, basis:total_rows, :] = jnp.zeros((total_rows - basis, LANES), jnp.float32)
        tail = second_sum.shape[1]
        second_sum[p, tail - 16 : tail, :] = jnp.zeros((16, LANES), jnp.float32)
        first_sum[p, 448:464, :] = jnp.zeros((16, LANES), jnp.float32)

    def mask(j, carry):
        rows = pl.ds(pl.multiple_of(j * width, width), width)
        keep = screen_ref[0, lax.rem(j, occ_blocks)].astype(jnp.float32)
        both[rows, :] = (both[rows, :].astype(jnp.float32) * keep).astype(both.dtype)
        return carry

    pair = []
    partner = device("x", 0, 1)
    flags.wait()
    for n in range(len(pieces)):
        loads[n].wait()
        lax.fori_loop(starts[n] // width, starts[n + 1] // width, mask, 0)
    for n in range(len(pieces)):
        if n == 0:
            pl.semaphore_wait(barrier, len(peers))
        pair.append(
            pltpu.make_async_remote_copy(
                src_ref=both.at[pl.ds(starts[n], pieces[n])],
                dst_ref=both.at[pl.ds(depth + starts[n], pieces[n])],
                send_sem=pair_send.at[n], recv_sem=pair_recv.at[n],
                device_id=partner, device_id_type=MESH,
            )
        )
        pair[-1].start()

    def turn(low, high):
        def one(m, carry):
            rows = pl.ds(pl.multiple_of(m * 256, 256), 256)
            for k in range(low, high, LANES):
                turned[rows, k : k + LANES] = both[k : k + LANES, rows].T
            return carry

        lax.fori_loop(0, basis // 256, one, 0)

    def multiply(tiles, low, high, fresh):
        tall = basis // 2
        columns = pl.ds(pl.multiple_of(core * half + tiles[0] * LANES, LANES), len(tiles) * LANES)

        def one(m, carry):
            rows = pl.ds(pl.multiple_of(m * tall, LANES), tall)
            value = jnp.dot(turned[rows, low:high], both[low:high, columns], preferred_element_type=jnp.float32)
            for n, p in enumerate(tiles):
                mine = value[:, n * LANES : (n + 1) * LANES]
                total[p, rows, :] = mine if fresh else total[p, rows, :] + mine
            return carry

        lax.fori_loop(0, 2, one, 0)

    def exponent(top):
        return jnp.floor(jnp.log(jnp.maximum(top, 1e-33)) * 1.4426950408889634) + 1.0

    def coded(value, power):
        return jnp.round(value * (jnp.exp2(-power) * TOP)).astype(jnp.int32).astype(jnp.int16)

    def put(ref, values):
        rows = lax.broadcasted_iota(jnp.int32, (HEAD, LANES), 0)
        head = jnp.zeros((HEAD, LANES), jnp.float32)
        for g, value in enumerate(values):
            power = exponent(jnp.max(jnp.abs(value), axis=0, keepdims=True))
            n = value.shape[0]
            ref[HEAD + g * n : HEAD + (g + 1) * n, :] = coded(value, power)
            head = jnp.where(rows == g, power, head)
        ref[0:HEAD, :] = head.astype(jnp.int32).astype(jnp.int16)

    def powers(ref):
        return jnp.exp2(ref[0:HEAD, :].astype(jnp.int32).astype(jnp.float32)) * (1.0 / TOP)

    def get(ref, scale, g, n):
        return ref[HEAD + g * n : HEAD + (g + 1) * n, :].astype(jnp.int32).astype(jnp.float32) * scale[g : g + 1, :]

    def group_rows(order):
        return 128 if order[0] == "z" else 112

    def load(p, order, block, c, g):
        if order[0] == "y":
            start = block * (8 * own * SIDE) + c * (4 * own * SIDE) + g * 112
            return total[p, pl.ds(pl.multiple_of(start, 8), 112), :]
        if order[0] in "xw":
            near, far = own * SIDE, 8 * own * SIDE
            if order[0] == "w":
                near, far = core * near + (1 - core) * far, (1 - core) * near + core * far
            starts = [(2 * g + n) * far + c * (4 * own * SIDE) + block * near for n in range(2)]
            return jnp.concatenate([total[p, pl.ds(pl.multiple_of(s, 8), 56), :] for s in starts], axis=0)
        starts = [
            (2 * g + n) * (8 * own * SIDE) + c * (4 * own * SIDE) + m * (own * SIDE) + block * own
            for n in range(2) for m in range(SIDE)
        ]
        return jnp.concatenate([total[p, pl.ds(s, 16), :] for s in starts], axis=0)

    def second_block(p, order, j):
        if order[1] == "z":
            starts = [c * (4 * own * SIDE) + m * (own * SIDE) + j * own for c in range(2) for m in range(SIDE)]
            return jnp.concatenate([first_sum[p, pl.ds(s, 16), :] for s in starts], axis=0)
        if order[0] != "z" or order[1] == "y":
            n = 64 if order[0] == "z" else 56
            starts = [c * 4 * n + j * n for c in range(2)]
        else:
            n = 16
            starts = [c * 256 + m * 64 + j * n for c in range(2) for m in range(SIDE)]
        return jnp.concatenate([first_sum[p, pl.ds(pl.multiple_of(s, 8), n), :] for s in starts], axis=0)

    def copy(here, there, a, b, to):
        return pltpu.make_async_remote_copy(
            src_ref=here, dst_ref=there, send_sem=a, recv_sem=b, device_id=to, device_id_type=MESH,
        )

    def sized(order, groups):
        return pl.ds(0, HEAD + groups * group_rows(order))

    def copy_one(p, s):
        order = orders[p]
        run = sized(order, 2)
        return copy(out_one.at[p, s, run], in_one.at[p, s, run], one_send.at[p, s], one_recv.at[p, s],
                    device(order[0], (1, 3)[s]))

    def copy_two(p, s, late):
        order = orders[p]
        run = sized(order, 2)
        n = 2 * s + late
        return copy(out_two.at[p, n, run], in_two.at[p, n, run], two_send.at[p, n], two_recv.at[p, n],
                    device(order[0], (1, 3)[s]))

    def second_rows(order):
        return 128 if "z" in order[:2] else 112

    def copy_three(p, d):
        order = orders[p]
        run = pl.ds(0, HEAD + second_rows(order))
        return copy(out_three.at[p, d - 1, run], in_three.at[p, d - 1, run], three_send.at[p, d - 1],
                    three_recv.at[p, d - 1], device(order[1], d))

    def copy_four(p, d, flip):
        s = 2 * d + flip - 1
        return copy(out_four.at[p, s], in_four.at[p, s], four_send.at[p, s], four_recv.at[p, s],
                    device(orders[p][2], d, flip))

    def step_one(p):
        order = orders[p]
        block = place(order[0], 2)
        for s in range(2):
            put(out_one.at[p, s], [load(p, order, block, s, g) for g in range(2)])
            copy_one(p, s).start()

    def step_solo(p):
        order = orders[p]
        for s in range(2):
            block = place(order[0], (1, 3)[s])
            put(out_two.at[p, 2 * s], [load(p, order, block, 1 - s, g) for g in range(2)])
            copy_two(p, s, 0).start()

    def step_two(p):
        order = orders[p]
        n = group_rows(order)
        for s in range(2):
            copy_one(p, s).wait_recv()
            block = place(order[0], (1, 3)[s])
            ref = in_one.at[p, s]
            scale = powers(ref)
            put(out_two.at[p, 2 * s + 1], [load(p, order, block, s, g) + get(ref, scale, g, n) for g in range(2)])
            copy_two(p, s, 1).start()

    def collect(p):
        order = orders[p]
        n = group_rows(order)
        for s in range(2):
            for late in range(2):
                copy_two(p, s, late).wait_recv()
        for c in range(2):
            refs = [in_two.at[p, 2 * s + (1 if c == s else 0)] for s in range(2)]
            scales = [powers(ref) for ref in refs]
            for g in range(2):
                value = load(p, order, at[order[0]], c, g)
                for ref, scale in zip(refs, scales):
                    value = value + get(ref, scale, g, n)
                first_sum[p, (2 * c + g) * n : (2 * c + g + 1) * n, :] = value

    def plane_rows(order, c, u, v):
        if order[0] == "z":
            steps = {"y": SIDE * 16, "x": 16} if order[1] == "y" else {"x": 16, "y": SIDE * 16}
            return pl.ds(pl.multiple_of(c * 256 + u * steps[order[1]] + v * steps[order[2]], 8), 16)
        step = own if order[1] == "z" else own * SIDE
        other = own * SIDE if order[1] == "z" else own
        return pl.ds(c * (4 * own * SIDE) + u * step + v * other, 16)

    def plane_slot(du, dv, flip):
        return (du * SIDE + dv) * 2 + flip - 1

    def step_plane(q):
        p = merged[q]
        order = orders[p]
        collect(p)
        row = lax.rem(lax.broadcasted_iota(jnp.int32, (SIDE * 16, LANES), 0), 16)
        for du in (2, 1, 3, 0):
            u = place(order[1], du)
            for flip in range(2):
                c = 1 - core if flip else core
                value = jnp.concatenate(
                    [first_sum[p, plane_rows(order, c, u, place(order[2], dv)), :] for dv in range(SIDE)], axis=0
                )
                power = exponent(jnp.max(jnp.abs(value), axis=0, keepdims=True))
                code = jnp.where(row == own, power, jnp.round(value * (jnp.exp2(-power) * TOP)))
                code = code.astype(jnp.int32).astype(jnp.int16)
                for dv in (2, 1, 3, 0):
                    if du or dv or flip:
                        n = plane_slot(du, dv, flip)
                        out_plane[q, n] = code[dv * 16 : (dv + 1) * 16, :]
                        copy(out_plane.at[q, n], in_plane.at[q, n], plane_send.at[q], plane_recv.at[q],
                             moved([(order[1], du), (order[2], dv)], flip)).start()

    def wait_plane(q, sent):
        whole = copy(out_plane.at[q], in_plane.at[q], plane_send.at[q], plane_recv.at[q], partner)
        whole.wait_send() if sent else whole.wait_recv()

    def end_plane(q):
        p = merged[q]
        order = orders[p]
        wait_plane(q, False)
        for flip in range(2):
            c = 1 - core if flip else core
            value = None
            if not flip:
                value = first_sum[p, plane_rows(order, core, at[order[1]], at[order[2]]), :]
            for du in range(SIDE):
                for dv in range(SIDE):
                    if du or dv or flip:
                        code = in_plane[q, plane_slot(du, dv, flip)].astype(jnp.int32).astype(jnp.float32)
                        term = code * (jnp.exp2(code[own : own + 1, :]) * (1.0 / TOP))
                        value = term if value is None else value + term
            columns = pl.ds(pl.multiple_of(c * half + p * LANES, LANES), LANES)
            out_ref[:, columns] = value[0:own, :]

    def step_three(p):
        order = orders[p]
        collect(p)
        for d in range(1, SIDE):
            put(out_three.at[p, d - 1], [second_block(p, order, place(order[1], d))])
            copy_three(p, d).start()

    def last_rows(order, c, k):
        if "z" in order[:2]:
            return pl.ds(pl.multiple_of(c * 64 + k * 16, 8), 16)
        return pl.ds(c * 4 * own + k * own, 16)

    def step_four(p):
        order = orders[p]
        n = second_rows(order)
        value = second_block(p, order, at[order[1]])
        for d in range(1, SIDE):
            copy_three(p, d).wait_recv()
            ref = in_three.at[p, d - 1]
            value = value + get(ref, powers(ref), 0, n)
        second_sum[p, 0:n, :] = value
        rows = lax.broadcasted_iota(jnp.int32, (16, LANES), 0)
        for d in range(SIDE):
            for flip in range(2):
                if d or flip:
                    c = 1 - core if flip else core
                    value = second_sum[p, last_rows(order, c, place(order[2], d)), :]
                    top = jnp.max(jnp.where(rows < own, jnp.abs(value), 0.0), axis=0, keepdims=True)
                    power = exponent(top)
                    code = jnp.round(value * (jnp.exp2(-power) * TOP))
                    code = jnp.where(rows < own, code, power)
                    out_four[p, 2 * d + flip - 1] = code.astype(jnp.int32).astype(jnp.int16)
                    copy_four(p, d, flip).start()

    def step_five(p):
        order = orders[p]
        for flip in range(2):
            c = 1 - core if flip else core
            value = None
            if not flip:
                value = second_sum[p, last_rows(order, core, at[order[2]]), :]
            for d in range(SIDE):
                if d or flip:
                    copy_four(p, d, flip).wait_recv()
                    code = in_four[p, 2 * d + flip - 1].astype(jnp.int32).astype(jnp.float32)
                    term = code * (jnp.exp2(code[own : own + 1, :]) * (1.0 / TOP))
                    value = term if value is None else value + term
            columns = pl.ds(pl.multiple_of(c * half + p * LANES, LANES), LANES)
            out_ref[:, columns] = value[0:own, :]

    first, rest = [0, 1, 2], [[3, 4, 5, 6]]
    merged = MERGED
    apart = [p for p in range(parts) if p not in merged]
    edges = [depth // LANES * LANES] + [depth + start for start in starts[1:]]
    turn(0, edges[0])
    multiply(first, 0, edges[0], True)
    pair[0].wait_recv()
    turn(edges[0], edges[1])
    multiply(first, edges[0], edges[1], False)
    for n in range(1, len(pieces)):
        pair[n].wait_recv()
        turn(edges[n], edges[n + 1])
    multiply(first, edges[1], 2 * depth, False)
    for p in first:
        step_one(p)
    for p in first:
        step_solo(p)
    late = rest[0]
    multiply(late, 0, 2 * depth, True)
    for p in late:
        step_one(p)
    for p in first:
        step_two(p)
    for p in late[:-1]:
        step_solo(p)
    for p in late[:-1]:
        step_two(p)
    step_solo(late[-1])
    step_two(late[-1])
    for p in first:
        step_three(p)
    for q in (1, 0, 2, 3):
        step_plane(q)
    for p in apart:
        step_four(p)
    for q in range(len(merged)):
        end_plane(q)
    for p in apart:
        step_five(p)

    for n in range(len(pieces)):
        pair[n].wait_send()
    for p in range(parts):
        for s in range(2):
            copy_one(p, s).wait_send()
            for late in range(2):
                copy_two(p, s, late).wait_send()
    for q in range(len(merged)):
        wait_plane(q, True)
    for p in apart:
        for d in range(SIDE):
            if d:
                copy_three(p, d).wait_send()
            for flip in range(2):
                if d or flip:
                    copy_four(p, d, flip).wait_send()


def solution(mesh):
    groups, members = mesh.shape["grp"], mesh.shape["mem"]

    def on_device(factors, screen):
        aux_rows, occ_count, basis = factors.shape
        depth = aux_rows * occ_count
        own = basis // (groups * members)
        parts = basis // 2 // LANES
        pieces = PIECES
        dma = pltpu.SemaphoreType.DMA
        vmem = pl.BlockSpec(memory_space=pltpu.VMEM)
        slots = 2 * SIDE - 1

        def codes(count, rows):
            return pltpu.VMEM((parts, count, rows, LANES), jnp.int16)

        return pl.pallas_call(
            functools.partial(kernel, members, occ_count // screen.shape[1], ORDERS, pieces),
            out_shape=jax.ShapeDtypeStruct((own, basis), jnp.float32),
            in_specs=[pl.BlockSpec(memory_space=pltpu.HBM)] * 2,
            out_specs=vmem,
            scratch_shapes=[
                pltpu.SMEM(screen.shape, jnp.int32),
                pltpu.VMEM((2 * depth, basis), jnp.bfloat16),
                pltpu.VMEM((basis, 2 * depth), jnp.bfloat16),
                pltpu.VMEM((parts, basis + 8, LANES), jnp.float32),
                pltpu.VMEM((parts, 512, LANES), jnp.float32),
                pltpu.VMEM((parts, 128, LANES), jnp.float32),
                codes(2, HEAD + 256), codes(2, HEAD + 256),
                codes(4, HEAD + 256), codes(4, HEAD + 256),
                codes(3, HEAD + 128), codes(3, HEAD + 128),
                codes(slots, 16), codes(slots, 16),
                pltpu.VMEM((len(MERGED), PLANE, 16, LANES), jnp.int16),
                pltpu.VMEM((len(MERGED), PLANE, 16, LANES), jnp.int16),
                dma, dma((len(pieces),)), dma((len(pieces),)), dma((len(pieces),)),
                dma((parts, 2)), dma((parts, 2)),
                dma((parts, 4)), dma((parts, 4)),
                dma((parts, 3)), dma((parts, 3)),
                dma((parts, slots)), dma((parts, slots)),
                dma((len(MERGED),)), dma((len(MERGED),)),
            ],
            compiler_params=pltpu.CompilerParams(
                collective_id=0, has_side_effects=True, vmem_limit_bytes=53 * 1024 * 1024
            ),
        )(
            pltpu.with_memory_space_constraint(factors.reshape(depth, basis), pltpu.HBM),
            pltpu.with_memory_space_constraint(screen, pltpu.HBM),
        )

    placed = (P(("grp", "mem"), None, None), P(("grp", "mem"), None))
    return jax.shard_map(
        on_device, mesh=mesh, in_specs=placed, out_specs=P(("grp", "mem"), None), check_vma=False
    )
```

```python
import functools

import jax
import jax.numpy as jnp
from jax import lax
from jax.experimental import pallas as pl
from jax.experimental.pallas import tpu as pltpu
from jax.sharding import PartitionSpec as P

LANES = 128
TOP = 32767.0
SIDE = 4
HEAD = 8
MESH = pl.DeviceIdType.MESH
ORDERS = ("yzx", "zxy", "xyz", "yzx", "zxy", "xyz", "wvz")
PIECES = (192, 256, 128)
MERGED = (3, 4, 5, 6)
PLANE = 2 * SIDE * SIDE - 1


def kernel(
    members, width, orders, pieces,
    x_ref, flags_ref, out_ref,
    screen_ref, both, turned, total, first_sum, second_sum,
    out_one, in_one, out_two, in_two, out_three, in_three, out_four, in_four, out_plane, in_plane,
    flag_sem, load_sem, pair_send, pair_recv, one_send, one_recv, two_send, two_recv,
    three_send, three_recv, four_send, four_recv, plane_send, plane_recv,
):
    depth, basis = x_ref.shape
    own = out_ref.shape[0]
    half = basis // 2
    parts = len(orders)
    occ_blocks = screen_ref.shape[1]
    grp, mem = lax.axis_index("grp"), lax.axis_index("mem")
    at = {"y": lax.div(grp, 2), "c": lax.rem(grp, 2), "x": lax.div(mem, SIDE), "z": lax.rem(mem, SIDE)}
    core = at["c"]

    at["w"] = (1 - core) * at["y"] + core * at["x"]
    at["v"] = core * at["y"] + (1 - core) * at["x"]

    def place(axis, d):
        return lax.rem(at[axis] + d, SIDE)

    def device(axis, d, flip=0):
        return moved([(axis, d)], flip)

    def moved(moves, flip=0):
        there = dict(at)
        for axis, d in moves:
            if d and axis in "wv":
                to = place(axis, d)
                on_y = 1 - core if axis == "w" else core
                there["y"] = on_y * to + (1 - on_y) * there["y"]
                there["x"] = (1 - on_y) * to + on_y * there["x"]
            elif d:
                there[axis] = place(axis, d)
        if flip:
            there["c"] = 1 - core
        return (there["y"] * 2 + there["c"], there["x"] * SIDE + there["z"])

    last_axes = sorted({order[2] for order in orders})
    peers = [device("x", 0, 1)]
    for axis in "xyz":
        for d in range(1, SIDE):
            peers.append(device(axis, d))
            if axis in last_axes:
                peers.append(device(axis, d, 1))
    barrier = pltpu.get_barrier_semaphore()
    for other in peers:
        pl.semaphore_signal(barrier, inc=1, device_id=other, device_id_type=MESH)

    starts = [sum(pieces[:n]) for n in range(len(pieces) + 1)]
    flags = pltpu.make_async_copy(flags_ref, screen_ref, flag_sem)
    flags.start()
    loads = []
    for n in range(len(pieces)):
        rows = pl.ds(starts[n], pieces[n])
        loads.append(pltpu.make_async_copy(x_ref.at[rows], both.at[rows], load_sem.at[n]))
        loads[-1].start()

    total_rows = total.shape[1]
    for p in range(parts):
        total[p, basis:total_rows, :] = jnp.zeros((total_rows - basis, LANES), jnp.float32)
        tail = second_sum.shape[1]
        second_sum[p, tail - 16 : tail, :] = jnp.zeros((16, LANES), jnp.float32)
        first_sum[p, 448:464, :] = jnp.zeros((16, LANES), jnp.float32)

    def mask(j, carry):
        rows = pl.ds(pl.multiple_of(j * width, width), width)
        keep = screen_ref[0, lax.rem(j, occ_blocks)].astype(jnp.float32)
        both[rows, :] = (both[rows, :].astype(jnp.float32) * keep).astype(both.dtype)
        return carry

    pair = []
    partner = device("x", 0, 1)
    flags.wait()
    for n in range(len(pieces)):
        loads[n].wait()
        lax.fori_loop(starts[n] // width, starts[n + 1] // width, mask, 0)
    for n in range(len(pieces)):
        if n == 0:
            pl.semaphore_wait(barrier, len(peers))
        pair.append(
            pltpu.make_async_remote_copy(
                src_ref=both.at[pl.ds(starts[n], pieces[n])],
                dst_ref=both.at[pl.ds(depth + starts[n], pieces[n])],
                send_sem=pair_send.at[n], recv_sem=pair_recv.at[n],
                device_id=partner, device_id_type=MESH,
            )
        )
        pair[-1].start()

    def turn(low, high):
        def one(m, carry):
            rows = pl.ds(pl.multiple_of(m * 256, 256), 256)
            for k in range(low, high, LANES):
                turned[rows, k : k + LANES] = both[k : k + LANES, rows].T
            return carry

        lax.fori_loop(0, basis // 256, one, 0)

    def multiply(tiles, low, high, fresh):
        tall = basis // 2
        columns = pl.ds(pl.multiple_of(core * half + tiles[0] * LANES, LANES), len(tiles) * LANES)

        def one(m, carry):
            rows = pl.ds(pl.multiple_of(m * tall, LANES), tall)
            value = jnp.dot(turned[rows, low:high], both[low:high, columns], preferred_element_type=jnp.float32)
            for n, p in enumerate(tiles):
                mine = value[:, n * LANES : (n + 1) * LANES]
                total[p, rows, :] = mine if fresh else total[p, rows, :] + mine
            return carry

        lax.fori_loop(0, 2, one, 0)

    def exponent(top):
        return jnp.floor(jnp.log(jnp.maximum(top, 1e-33)) * 1.4426950408889634) + 1.0

    def coded(value, power):
        return jnp.round(value * (jnp.exp2(-power) * TOP)).astype(jnp.int32).astype(jnp.int16)

    def put(ref, values):
        rows = lax.broadcasted_iota(jnp.int32, (HEAD, LANES), 0)
        head = jnp.zeros((HEAD, LANES), jnp.float32)
        end = sum(value.shape[0] for value in values)
        for g, value in enumerate(values):
            power = exponent(jnp.max(jnp.abs(value), axis=0, keepdims=True))
            n = value.shape[0]
            ref[g * n : (g + 1) * n, :] = coded(value, power)
            head = jnp.where(rows == g, power, head)
        ref[end : end + HEAD, :] = head.astype(jnp.int32).astype(jnp.int16)

    def powers(ref, end):
        return jnp.exp2(ref[end : end + HEAD, :].astype(jnp.int32).astype(jnp.float32)) * (1.0 / TOP)

    def get(ref, scale, g, n):
        return ref[g * n : (g + 1) * n, :].astype(jnp.int32).astype(jnp.float32) * scale[g : g + 1, :]

    def group_rows(order):
        return 128 if order[0] == "z" else 112

    def load(p, order, block, c, g):
        if order[0] == "y":
            start = block * (8 * own * SIDE) + c * (4 * own * SIDE) + g * 112
            return total[p, pl.ds(pl.multiple_of(start, 8), 112), :]
        if order[0] in "xw":
            near, far = own * SIDE, 8 * own * SIDE
            if order[0] == "w":
                near, far = core * near + (1 - core) * far, (1 - core) * near + core * far
            starts = [(2 * g + n) * far + c * (4 * own * SIDE) + block * near for n in range(2)]
            return jnp.concatenate([total[p, pl.ds(pl.multiple_of(s, 8), 56), :] for s in starts], axis=0)
        starts = [
            (2 * g + n) * (8 * own * SIDE) + c * (4 * own * SIDE) + m * (own * SIDE) + block * own
            for n in range(2) for m in range(SIDE)
        ]
        return jnp.concatenate([total[p, pl.ds(s, 16), :] for s in starts], axis=0)

    def second_block(p, order, j):
        if order[1] == "z":
            starts = [c * (4 * own * SIDE) + m * (own * SIDE) + j * own for c in range(2) for m in range(SIDE)]
            return jnp.concatenate([first_sum[p, pl.ds(s, 16), :] for s in starts], axis=0)
        if order[0] != "z" or order[1] == "y":
            n = 64 if order[0] == "z" else 56
            starts = [c * 4 * n + j * n for c in range(2)]
        else:
            n = 16
            starts = [c * 256 + m * 64 + j * n for c in range(2) for m in range(SIDE)]
        return jnp.concatenate([first_sum[p, pl.ds(pl.multiple_of(s, 8), n), :] for s in starts], axis=0)

    def copy(here, there, a, b, to):
        return pltpu.make_async_remote_copy(
            src_ref=here, dst_ref=there, send_sem=a, recv_sem=b, device_id=to, device_id_type=MESH,
        )

    def sized(order, groups):
        return pl.ds(0, HEAD + groups * group_rows(order))

    def copy_one(p, s):
        order = orders[p]
        run = sized(order, 2)
        return copy(out_one.at[p, s, run], in_one.at[p, s, run], one_send.at[p, s], one_recv.at[p, s],
                    device(order[0], (1, 3)[s]))

    def copy_two(p, s, late):
        order = orders[p]
        run = sized(order, 2)
        n = 2 * s + late
        return copy(out_two.at[p, n, run], in_two.at[p, n, run], two_send.at[p, n], two_recv.at[p, n],
                    device(order[0], (1, 3)[s]))

    def second_rows(order):
        return 128 if "z" in order[:2] else 112

    def copy_three(p, d):
        order = orders[p]
        run = pl.ds(0, HEAD + second_rows(order))
        return copy(out_three.at[p, d - 1, run], in_three.at[p, d - 1, run], three_send.at[p, d - 1],
                    three_recv.at[p, d - 1], device(order[1], d))

    def copy_four(p, d, flip):
        s = 2 * d + flip - 1
        return copy(out_four.at[p, s], in_four.at[p, s], four_send.at[p, s], four_recv.at[p, s],
                    device(orders[p][2], d, flip))

    def step_one(p):
        order = orders[p]
        block = place(order[0], 2)
        for s in range(2):
            put(out_one.at[p, s], [load(p, order, block, s, g) for g in range(2)])
            copy_one(p, s).start()

    def step_solo(p):
        order = orders[p]
        for s in range(2):
            block = place(order[0], (1, 3)[s])
            put(out_two.at[p, 2 * s], [load(p, order, block, 1 - s, g) for g in range(2)])
            copy_two(p, s, 0).start()

    def step_two(p):
        order = orders[p]
        n = group_rows(order)
        for s in range(2):
            copy_one(p, s).wait_recv()
            block = place(order[0], (1, 3)[s])
            ref = in_one.at[p, s]
            scale = powers(ref, 2 * n)
            put(out_two.at[p, 2 * s + 1], [load(p, order, block, s, g) + get(ref, scale, g, n) for g in range(2)])
            copy_two(p, s, 1).start()

    def collect(p):
        order = orders[p]
        n = group_rows(order)
        for s in range(2):
            for late in range(2):
                copy_two(p, s, late).wait_recv()
        for c in range(2):
            refs = [in_two.at[p, 2 * s + (1 if c == s else 0)] for s in range(2)]
            scales = [powers(ref, 2 * n) for ref in refs]
            for g in range(2):
                value = load(p, order, at[order[0]], c, g)
                for ref, scale in zip(refs, scales):
                    value = value + get(ref, scale, g, n)
                first_sum[p, (2 * c + g) * n : (2 * c + g + 1) * n, :] = value

    def plane_rows(order, c, u, v):
        if order[0] == "z":
            steps = {"y": SIDE * 16, "x": 16} if order[1] == "y" else {"x": 16, "y": SIDE * 16}
            return pl.ds(pl.multiple_of(c * 256 + u * steps[order[1]] + v * steps[order[2]], 8), 16)
        step = own if order[1] == "z" else own * SIDE
        other = own * SIDE if order[1] == "z" else own
        return pl.ds(c * (4 * own * SIDE) + u * step + v * other, 16)

    def plane_slot(du, dv, flip):
        return (du * SIDE + dv) * 2 + flip - 1

    def step_plane(q):
        p = merged[q]
        order = orders[p]
        collect(p)
        row = lax.rem(lax.broadcasted_iota(jnp.int32, (SIDE * 16, LANES), 0), 16)
        for du in (2, 1, 3, 0):
            u = place(order[1], du)
            for flip in range(2):
                c = 1 - core if flip else core
                value = jnp.concatenate(
                    [first_sum[p, plane_rows(order, c, u, place(order[2], dv)), :] for dv in range(SIDE)], axis=0
                )
                power = exponent(jnp.max(jnp.abs(value), axis=0, keepdims=True))
                code = jnp.where(row == own, power, jnp.round(value * (jnp.exp2(-power) * TOP)))
                code = code.astype(jnp.int32).astype(jnp.int16)
                for dv in (2, 1, 3, 0):
                    if du or dv or flip:
                        n = plane_slot(du, dv, flip)
                        out_plane[q, n] = code[dv * 16 : (dv + 1) * 16, :]
                        copy(out_plane.at[q, n], in_plane.at[q, n], plane_send.at[q], plane_recv.at[q],
                             moved([(order[1], du), (order[2], dv)], flip)).start()

    def wait_plane(q, sent):
        whole = copy(out_plane.at[q], in_plane.at[q], plane_send.at[q], plane_recv.at[q], partner)
        whole.wait_send() if sent else whole.wait_recv()

    def end_plane(q):
        p = merged[q]
        order = orders[p]
        wait_plane(q, False)
        for flip in range(2):
            c = 1 - core if flip else core
            value = None
            if not flip:
                value = first_sum[p, plane_rows(order, core, at[order[1]], at[order[2]]), :]
            for du in range(SIDE):
                for dv in range(SIDE):
                    if du or dv or flip:
                        code = in_plane[q, plane_slot(du, dv, flip)].astype(jnp.int32).astype(jnp.float32)
                        term = code * (jnp.exp2(code[own : own + 1, :]) * (1.0 / TOP))
                        value = term if value is None else value + term
            columns = pl.ds(pl.multiple_of(c * half + p * LANES, LANES), LANES)
            out_ref[:, columns] = value[0:own, :]

    def step_three(p):
        order = orders[p]
        collect(p)
        for d in range(1, SIDE):
            put(out_three.at[p, d - 1], [second_block(p, order, place(order[1], d))])
            copy_three(p, d).start()

    def last_rows(order, c, k):
        if "z" in order[:2]:
            return pl.ds(pl.multiple_of(c * 64 + k * 16, 8), 16)
        return pl.ds(c * 4 * own + k * own, 16)

    def step_four(p):
        order = orders[p]
        n = second_rows(order)
        value = second_block(p, order, at[order[1]])
        for d in range(1, SIDE):
            copy_three(p, d).wait_recv()
            ref = in_three.at[p, d - 1]
            value = value + get(ref, powers(ref, n), 0, n)
        second_sum[p, 0:n, :] = value
        rows = lax.broadcasted_iota(jnp.int32, (16, LANES), 0)
        for d in range(SIDE):
            for flip in range(2):
                if d or flip:
                    c = 1 - core if flip else core
                    value = second_sum[p, last_rows(order, c, place(order[2], d)), :]
                    top = jnp.max(jnp.where(rows < own, jnp.abs(value), 0.0), axis=0, keepdims=True)
                    power = exponent(top)
                    code = jnp.round(value * (jnp.exp2(-power) * TOP))
                    code = jnp.where(rows < own, code, power)
                    out_four[p, 2 * d + flip - 1] = code.astype(jnp.int32).astype(jnp.int16)
                    copy_four(p, d, flip).start()

    def step_five(p):
        order = orders[p]
        for flip in range(2):
            c = 1 - core if flip else core
            value = None
            if not flip:
                value = second_sum[p, last_rows(order, core, at[order[2]]), :]
            for d in range(SIDE):
                if d or flip:
                    copy_four(p, d, flip).wait_recv()
                    code = in_four[p, 2 * d + flip - 1].astype(jnp.int32).astype(jnp.float32)
                    term = code * (jnp.exp2(code[own : own + 1, :]) * (1.0 / TOP))
                    value = term if value is None else value + term
            columns = pl.ds(pl.multiple_of(c * half + p * LANES, LANES), LANES)
            out_ref[:, columns] = value[0:own, :]

    first, rest = [0, 1, 2], [[3, 4, 5, 6]]
    merged = MERGED
    apart = [p for p in range(parts) if p not in merged]
    edges = [depth // LANES * LANES] + [depth + start for start in starts[1:]]
    turn(0, edges[0])
    multiply(first, 0, edges[0], True)
    pair[0].wait_recv()
    turn(edges[0], edges[1])
    multiply(first, edges[0], edges[1], False)
    for n in range(1, len(pieces)):
        pair[n].wait_recv()
        turn(edges[n], edges[n + 1])
    multiply(first, edges[1], 2 * depth, False)
    for p in first:
        step_one(p)
    for p in first:
        step_solo(p)
    late = rest[0]
    multiply(late, 0, 2 * depth, True)
    for p in late:
        step_one(p)
    for p in first:
        step_two(p)
    for p in late[:-1]:
        step_solo(p)
    for p in late[:-1]:
        step_two(p)
    step_solo(late[-1])
    step_two(late[-1])
    for p in first:
        step_three(p)
    for q in (1, 0, 2, 3):
        step_plane(q)
    for p in apart:
        step_four(p)
    for n in range(len(pieces)):
        pair[n].wait_send()
    for p in range(parts):
        for s in range(2):
            copy_one(p, s).wait_send()
            for late_half in range(2):
                copy_two(p, s, late_half).wait_send()
    for p in apart:
        for d in range(1, SIDE):
            copy_three(p, d).wait_send()
    for q in (1, 0, 2, 3):
        end_plane(q)
    for p in apart:
        step_five(p)
    for q in range(len(merged)):
        wait_plane(q, True)
    for p in apart:
        for d in range(SIDE):
            for flip in range(2):
                if d or flip:
                    copy_four(p, d, flip).wait_send()


def solution(mesh):
    groups, members = mesh.shape["grp"], mesh.shape["mem"]

    def on_device(factors, screen):
        aux_rows, occ_count, basis = factors.shape
        depth = aux_rows * occ_count
        own = basis // (groups * members)
        parts = basis // 2 // LANES
        pieces = PIECES
        dma = pltpu.SemaphoreType.DMA
        vmem = pl.BlockSpec(memory_space=pltpu.VMEM)
        slots = 2 * SIDE - 1

        def codes(count, rows):
            return pltpu.VMEM((parts, count, rows, LANES), jnp.int16)

        return pl.pallas_call(
            functools.partial(kernel, members, occ_count // screen.shape[1], ORDERS, pieces),
            out_shape=jax.ShapeDtypeStruct((own, basis), jnp.float32),
            in_specs=[pl.BlockSpec(memory_space=pltpu.HBM)] * 2,
            out_specs=vmem,
            scratch_shapes=[
                pltpu.SMEM(screen.shape, jnp.int32),
                pltpu.VMEM((2 * depth, basis), jnp.bfloat16),
                pltpu.VMEM((basis, 2 * depth), jnp.bfloat16),
                pltpu.VMEM((parts, basis + 8, LANES), jnp.float32),
                pltpu.VMEM((parts, 512, LANES), jnp.float32),
                pltpu.VMEM((parts, 128, LANES), jnp.float32),
                codes(2, HEAD + 256), codes(2, HEAD + 256),
                codes(4, HEAD + 256), codes(4, HEAD + 256),
                codes(3, HEAD + 128), codes(3, HEAD + 128),
                codes(slots, 16), codes(slots, 16),
                pltpu.VMEM((len(MERGED), PLANE, 16, LANES), jnp.int16),
                pltpu.VMEM((len(MERGED), PLANE, 16, LANES), jnp.int16),
                dma, dma((len(pieces),)), dma((len(pieces),)), dma((len(pieces),)),
                dma((parts, 2)), dma((parts, 2)),
                dma((parts, 4)), dma((parts, 4)),
                dma((parts, 3)), dma((parts, 3)),
                dma((parts, slots)), dma((parts, slots)),
                dma((len(MERGED),)), dma((len(MERGED),)),
            ],
            compiler_params=pltpu.CompilerParams(
                collective_id=0, has_side_effects=True, vmem_limit_bytes=53 * 1024 * 1024
            ),
        )(
            pltpu.with_memory_space_constraint(factors.reshape(depth, basis), pltpu.HBM),
            pltpu.with_memory_space_constraint(screen, pltpu.HBM),
        )

    placed = (P(("grp", "mem"), None, None), P(("grp", "mem"), None))
    return jax.shard_map(
        on_device, mesh=mesh, in_specs=placed, out_specs=P(("grp", "mem"), None), check_vma=False
    )
```

```python
import functools

import jax
import jax.numpy as jnp
from jax import lax
from jax.experimental import pallas as pl
from jax.experimental.pallas import tpu as pltpu
from jax.sharding import PartitionSpec as P

LANES = 128
TOP = 32767.0
SIDE = 4
HEAD = 8
MESH = pl.DeviceIdType.MESH
ORDERS = ("yzx", "zxy", "xyz", "yzx", "zxy", "xyz", "wvz")
PIECES = (192, 256, 128)
MERGED = (3, 4, 5, 6)
PLANE = 2 * SIDE * SIDE - 1


def kernel(
    members, width, orders, pieces,
    x_ref, flags_ref, out_ref,
    screen_ref, both, turned, total, first_sum, second_sum,
    out_one, in_one, out_two, in_two, out_three, in_three, out_four, in_four, out_plane, in_plane,
    flag_sem, load_sem, pair_send, pair_recv, one_send, one_recv, two_send, two_recv,
    three_send, three_recv, four_send, four_recv, plane_send, plane_recv,
):
    depth, basis = x_ref.shape
    own = out_ref.shape[0]
    half = basis // 2
    parts = len(orders)
    occ_blocks = screen_ref.shape[1]
    grp, mem = lax.axis_index("grp"), lax.axis_index("mem")
    at = {"y": lax.div(grp, 2), "c": lax.rem(grp, 2), "x": lax.div(mem, SIDE), "z": lax.rem(mem, SIDE)}
    core = at["c"]

    at["w"] = (1 - core) * at["y"] + core * at["x"]
    at["v"] = core * at["y"] + (1 - core) * at["x"]

    def place(axis, d):
        return lax.rem(at[axis] + d, SIDE)

    def device(axis, d, flip=0):
        return moved([(axis, d)], flip)

    def moved(moves, flip=0):
        there = dict(at)
        for axis, d in moves:
            if d and axis in "wv":
                to = place(axis, d)
                on_y = 1 - core if axis == "w" else core
                there["y"] = on_y * to + (1 - on_y) * there["y"]
                there["x"] = (1 - on_y) * to + on_y * there["x"]
            elif d:
                there[axis] = place(axis, d)
        if flip:
            there["c"] = 1 - core
        return (there["y"] * 2 + there["c"], there["x"] * SIDE + there["z"])

    last_axes = sorted({order[2] for order in orders})
    peers = [device("x", 0, 1)]
    for axis in "xyz":
        for d in range(1, SIDE):
            peers.append(device(axis, d))
            if axis in last_axes:
                peers.append(device(axis, d, 1))
    barrier = pltpu.get_barrier_semaphore()
    for other in peers:
        pl.semaphore_signal(barrier, inc=1, device_id=other, device_id_type=MESH)

    starts = [sum(pieces[:n]) for n in range(len(pieces) + 1)]
    flags = pltpu.make_async_copy(flags_ref, screen_ref, flag_sem)
    flags.start()
    loads = []
    for n in range(len(pieces)):
        rows = pl.ds(starts[n], pieces[n])
        loads.append(pltpu.make_async_copy(x_ref.at[rows], both.at[rows], load_sem.at[n]))
        loads[-1].start()

    total_rows = total.shape[1]
    for p in range(parts):
        total[p, basis:total_rows, :] = jnp.zeros((total_rows - basis, LANES), jnp.float32)
        tail = second_sum.shape[1]
        second_sum[p, tail - 16 : tail, :] = jnp.zeros((16, LANES), jnp.float32)
        first_sum[p, 448:464, :] = jnp.zeros((16, LANES), jnp.float32)

    def mask(j, carry):
        rows = pl.ds(pl.multiple_of(j * width, width), width)
        keep = screen_ref[0, lax.rem(j, occ_blocks)].astype(jnp.float32)
        both[rows, :] = (both[rows, :].astype(jnp.float32) * keep).astype(both.dtype)
        return carry

    pair = []
    partner = device("x", 0, 1)
    flags.wait()
    for n in range(len(pieces)):
        loads[n].wait()
        lax.fori_loop(starts[n] // width, starts[n + 1] // width, mask, 0)
    for n in range(len(pieces)):
        if n == 0:
            pl.semaphore_wait(barrier, len(peers))
        pair.append(
            pltpu.make_async_remote_copy(
                src_ref=both.at[pl.ds(starts[n], pieces[n])],
                dst_ref=both.at[pl.ds(depth + starts[n], pieces[n])],
                send_sem=pair_send.at[n], recv_sem=pair_recv.at[n],
                device_id=partner, device_id_type=MESH,
            )
        )
        pair[-1].start()

    def turn(low, high):
        def one(m, carry):
            rows = pl.ds(pl.multiple_of(m * 256, 256), 256)
            for k in range(low, high, LANES):
                turned[rows, k : k + LANES] = both[k : k + LANES, rows].T
            return carry

        lax.fori_loop(0, basis // 256, one, 0)

    def multiply(tiles, low, high, fresh):
        tall = basis // 2
        columns = pl.ds(pl.multiple_of(core * half + tiles[0] * LANES, LANES), len(tiles) * LANES)

        def one(m, carry):
            rows = pl.ds(pl.multiple_of(m * tall, LANES), tall)
            value = jnp.dot(turned[rows, low:high], both[low:high, columns], preferred_element_type=jnp.float32)
            for n, p in enumerate(tiles):
                mine = value[:, n * LANES : (n + 1) * LANES]
                total[p, rows, :] = mine if fresh else total[p, rows, :] + mine
            return carry

        lax.fori_loop(0, 2, one, 0)

    def exponent(top):
        return jnp.floor(jnp.log(jnp.maximum(top, 1e-33)) * 1.4426950408889634) + 1.0

    def coded(value, power):
        return jnp.round(value * (jnp.exp2(-power) * TOP)).astype(jnp.int32).astype(jnp.int16)

    def put(ref, values):
        rows = lax.broadcasted_iota(jnp.int32, (HEAD, LANES), 0)
        head = jnp.zeros((HEAD, LANES), jnp.float32)
        end = sum(value.shape[0] for value in values)
        for g, value in enumerate(values):
            power = exponent(jnp.max(jnp.abs(value), axis=0, keepdims=True))
            n = value.shape[0]
            ref[g * n : (g + 1) * n, :] = coded(value, power)
            head = jnp.where(rows == g, power, head)
        ref[end : end + HEAD, :] = head.astype(jnp.int32).astype(jnp.int16)

    def powers(ref, end):
        return jnp.exp2(ref[end : end + HEAD, :].astype(jnp.int32).astype(jnp.float32)) * (1.0 / TOP)

    def get(ref, scale, g, n):
        return ref[g * n : (g + 1) * n, :].astype(jnp.int32).astype(jnp.float32) * scale[g : g + 1, :]

    def group_rows(order):
        return 128 if order[0] == "z" else 112

    def load(p, order, block, c, g):
        if order[0] == "y":
            start = block * (8 * own * SIDE) + c * (4 * own * SIDE) + g * 112
            return total[p, pl.ds(pl.multiple_of(start, 8), 112), :]
        if order[0] in "xw":
            near, far = own * SIDE, 8 * own * SIDE
            if order[0] == "w":
                near, far = core * near + (1 - core) * far, (1 - core) * near + core * far
            starts = [(2 * g + n) * far + c * (4 * own * SIDE) + block * near for n in range(2)]
            return jnp.concatenate([total[p, pl.ds(pl.multiple_of(s, 8), 56), :] for s in starts], axis=0)
        starts = [
            (2 * g + n) * (8 * own * SIDE) + c * (4 * own * SIDE) + m * (own * SIDE) + block * own
            for n in range(2) for m in range(SIDE)
        ]
        return jnp.concatenate([total[p, pl.ds(s, 16), :] for s in starts], axis=0)

    def second_block(p, order, j):
        if order[1] == "z":
            starts = [c * (4 * own * SIDE) + m * (own * SIDE) + j * own for c in range(2) for m in range(SIDE)]
            return jnp.concatenate([first_sum[p, pl.ds(s, 16), :] for s in starts], axis=0)
        if order[0] != "z" or order[1] == "y":
            n = 64 if order[0] == "z" else 56
            starts = [c * 4 * n + j * n for c in range(2)]
        else:
            n = 16
            starts = [c * 256 + m * 64 + j * n for c in range(2) for m in range(SIDE)]
        return jnp.concatenate([first_sum[p, pl.ds(pl.multiple_of(s, 8), n), :] for s in starts], axis=0)

    def copy(here, there, a, b, to):
        return pltpu.make_async_remote_copy(
            src_ref=here, dst_ref=there, send_sem=a, recv_sem=b, device_id=to, device_id_type=MESH,
        )

    def sized(order, groups):
        return pl.ds(0, HEAD + groups * group_rows(order))

    def copy_one(p, s):
        order = orders[p]
        run = sized(order, 2)
        return copy(out_one.at[p, s, run], in_one.at[p, s, run], one_send.at[p, s], one_recv.at[p, s],
                    device(order[0], (1, 3)[s]))

    def copy_two(p, s, late):
        order = orders[p]
        run = sized(order, 2)
        n = 2 * s + late
        return copy(out_two.at[p, n, run], in_two.at[p, n, run], two_send.at[p, n], two_recv.at[p, n],
                    device(order[0], (1, 3)[s]))

    def second_rows(order):
        return 128 if "z" in order[:2] else 112

    def copy_three(p, d):
        order = orders[p]
        run = pl.ds(0, HEAD + second_rows(order))
        return copy(out_three.at[p, d - 1, run], in_three.at[p, d - 1, run], three_send.at[p, d - 1],
                    three_recv.at[p, d - 1], device(order[1], d))

    def copy_four(p, d, flip):
        s = 2 * d + flip - 1
        return copy(out_four.at[p, s], in_four.at[p, s], four_send.at[p, s], four_recv.at[p, s],
                    device(orders[p][2], d, flip))

    def step_one(p):
        order = orders[p]
        block = place(order[0], 2)
        for s in range(2):
            put(out_one.at[p, s], [load(p, order, block, s, g) for g in range(2)])
            copy_one(p, s).start()

    def step_solo(p):
        order = orders[p]
        for s in range(2):
            block = place(order[0], (1, 3)[s])
            put(out_two.at[p, 2 * s], [load(p, order, block, 1 - s, g) for g in range(2)])
            copy_two(p, s, 0).start()

    def step_two(p):
        order = orders[p]
        n = group_rows(order)
        for s in range(2):
            copy_one(p, s).wait_recv()
            block = place(order[0], (1, 3)[s])
            ref = in_one.at[p, s]
            scale = powers(ref, 2 * n)
            put(out_two.at[p, 2 * s + 1], [load(p, order, block, s, g) + get(ref, scale, g, n) for g in range(2)])
            copy_two(p, s, 1).start()

    def collect(p):
        order = orders[p]
        n = group_rows(order)
        for s in range(2):
            for late in range(2):
                copy_two(p, s, late).wait_recv()
        for c in range(2):
            refs = [in_two.at[p, 2 * s + (1 if c == s else 0)] for s in range(2)]
            scales = [powers(ref, 2 * n) for ref in refs]
            for g in range(2):
                value = load(p, order, at[order[0]], c, g)
                for ref, scale in zip(refs, scales):
                    value = value + get(ref, scale, g, n)
                first_sum[p, (2 * c + g) * n : (2 * c + g + 1) * n, :] = value

    def plane_rows(order, c, u, v):
        if order[0] == "z":
            steps = {"y": SIDE * 16, "x": 16} if order[1] == "y" else {"x": 16, "y": SIDE * 16}
            return pl.ds(pl.multiple_of(c * 256 + u * steps[order[1]] + v * steps[order[2]], 8), 16)
        step = own if order[1] == "z" else own * SIDE
        other = own * SIDE if order[1] == "z" else own
        return pl.ds(c * (4 * own * SIDE) + u * step + v * other, 16)

    def plane_slot(du, dv, flip):
        return (du * SIDE + dv) * 2 + flip - 1

    def step_plane(q):
        p = merged[q]
        order = orders[p]
        collect(p)
        row = lax.rem(lax.broadcasted_iota(jnp.int32, (SIDE * 16, LANES), 0), 16)
        for du in (2, 1, 3, 0):
            u = place(order[1], du)
            for flip in range(2):
                c = 1 - core if flip else core
                value = jnp.concatenate(
                    [first_sum[p, plane_rows(order, c, u, place(order[2], dv)), :] for dv in range(SIDE)], axis=0
                )
                power = exponent(jnp.max(jnp.abs(value), axis=0, keepdims=True))
                code = jnp.where(row == own, power, jnp.round(value * (jnp.exp2(-power) * TOP)))
                code = code.astype(jnp.int32).astype(jnp.int16)
                for dv in (2, 1, 3, 0):
                    if du or dv or flip:
                        n = plane_slot(du, dv, flip)
                        out_plane[q, n] = code[dv * 16 : (dv + 1) * 16, :]
                        copy(out_plane.at[q, n], in_plane.at[q, n], plane_send.at[q], plane_recv.at[q],
                             moved([(order[1], du), (order[2], dv)], flip)).start()

    def wait_plane(q, sent):
        whole = copy(out_plane.at[q], in_plane.at[q], plane_send.at[q], plane_recv.at[q], partner)
        whole.wait_send() if sent else whole.wait_recv()

    def end_plane(q):
        p = merged[q]
        order = orders[p]
        wait_plane(q, False)
        for flip in range(2):
            c = 1 - core if flip else core
            value = None
            if not flip:
                value = first_sum[p, plane_rows(order, core, at[order[1]], at[order[2]]), :]
            for du in range(SIDE):
                for dv in range(SIDE):
                    if du or dv or flip:
                        code = in_plane[q, plane_slot(du, dv, flip)].astype(jnp.int32).astype(jnp.float32)
                        term = code * (jnp.exp2(code[own : own + 1, :]) * (1.0 / TOP))
                        value = term if value is None else value + term
            columns = pl.ds(pl.multiple_of(c * half + p * LANES, LANES), LANES)
            out_ref[:, columns] = value[0:own, :]

    def step_three(p):
        order = orders[p]
        collect(p)
        for d in range(1, SIDE):
            put(out_three.at[p, d - 1], [second_block(p, order, place(order[1], d))])
            copy_three(p, d).start()

    def last_rows(order, c, k):
        if "z" in order[:2]:
            return pl.ds(pl.multiple_of(c * 64 + k * 16, 8), 16)
        return pl.ds(c * 4 * own + k * own, 16)

    def step_four(p):
        order = orders[p]
        n = second_rows(order)
        value = second_block(p, order, at[order[1]])
        for d in range(1, SIDE):
            copy_three(p, d).wait_recv()
            ref = in_three.at[p, d - 1]
            value = value + get(ref, powers(ref, n), 0, n)
        second_sum[p, 0:n, :] = value
        rows = lax.broadcasted_iota(jnp.int32, (16, LANES), 0)
        for d in range(SIDE):
            for flip in range(2):
                if d or flip:
                    c = 1 - core if flip else core
                    value = second_sum[p, last_rows(order, c, place(order[2], d)), :]
                    top = jnp.max(jnp.where(rows < own, jnp.abs(value), 0.0), axis=0, keepdims=True)
                    power = exponent(top)
                    code = jnp.round(value * (jnp.exp2(-power) * TOP))
                    code = jnp.where(rows < own, code, power)
                    out_four[p, 2 * d + flip - 1] = code.astype(jnp.int32).astype(jnp.int16)
                    copy_four(p, d, flip).start()

    def step_five(p):
        order = orders[p]
        for flip in range(2):
            c = 1 - core if flip else core
            value = None
            if not flip:
                value = second_sum[p, last_rows(order, core, at[order[2]]), :]
            for d in range(SIDE):
                if d or flip:
                    copy_four(p, d, flip).wait_recv()
                    code = in_four[p, 2 * d + flip - 1].astype(jnp.int32).astype(jnp.float32)
                    term = code * (jnp.exp2(code[own : own + 1, :]) * (1.0 / TOP))
                    value = term if value is None else value + term
            columns = pl.ds(pl.multiple_of(c * half + p * LANES, LANES), LANES)
            out_ref[:, columns] = value[0:own, :]

    first, rest = [0, 1, 2], [[3, 4, 5, 6]]
    merged = MERGED
    apart = [p for p in range(parts) if p not in merged]
    edges = [depth // LANES * LANES] + [depth + start for start in starts[1:]]
    turn(0, edges[0])
    multiply(first, 0, edges[0], True)
    pair[0].wait_recv()
    turn(edges[0], edges[1])
    multiply(first, edges[0], edges[1], False)
    for n in range(1, len(pieces)):
        pair[n].wait_recv()
        turn(edges[n], edges[n + 1])
    multiply(first, edges[1], 2 * depth, False)
    for p in first:
        step_one(p)
    for p in first:
        step_solo(p)
    late = rest[0]
    multiply(late, 0, 2 * depth, True)
    for p in late:
        step_one(p)
    for p in first:
        step_two(p)
    for p in late[:-1]:
        step_solo(p)
    for p in late[:-1]:
        step_two(p)
    step_solo(late[-1])
    step_two(late[-1])
    for p in first:
        step_three(p)
    for q in (1, 0, 2, 3):
        step_plane(q)
    for p in apart:
        step_four(p)
    for n in range(len(pieces)):
        pair[n].wait_send()
    for p in range(parts):
        for s in range(2):
            copy_one(p, s).wait_send()
            for late_half in range(2):
                copy_two(p, s, late_half).wait_send()
    for p in apart:
        for d in range(1, SIDE):
            copy_three(p, d).wait_send()
    for q in (1, 0, 2, 3):
        end_plane(q)
    for p in apart:
        step_five(p)
    for q in range(len(merged)):
        wait_plane(q, True)
    for p in apart:
        for d in range(SIDE):
            for flip in range(2):
                if d or flip:
                    copy_four(p, d, flip).wait_send()


def solution(mesh):
    groups, members = mesh.shape["grp"], mesh.shape["mem"]

    def on_device(factors, screen):
        aux_rows, occ_count, basis = factors.shape
        depth = aux_rows * occ_count
        own = basis // (groups * members)
        parts = basis // 2 // LANES
        pieces = PIECES
        dma = pltpu.SemaphoreType.DMA
        vmem = pl.BlockSpec(memory_space=pltpu.VMEM)
        slots = 2 * SIDE - 1

        def codes(count, rows):
            return pltpu.VMEM((parts, count, rows, LANES), jnp.int16)

        return pl.pallas_call(
            functools.partial(kernel, members, occ_count // screen.shape[1], ORDERS, pieces),
            out_shape=jax.ShapeDtypeStruct((own, basis), jnp.float32),
            in_specs=[pl.BlockSpec(memory_space=pltpu.HBM)] * 2,
            out_specs=vmem,
            scratch_shapes=[
                pltpu.SMEM(screen.shape, jnp.int32),
                pltpu.VMEM((2 * depth, basis), jnp.bfloat16),
                pltpu.VMEM((basis, 2 * depth), jnp.bfloat16),
                pltpu.VMEM((parts, basis + 8, LANES), jnp.float32),
                pltpu.VMEM((parts, 512, LANES), jnp.float32),
                pltpu.VMEM((parts, 128, LANES), jnp.float32),
                codes(2, 16 + 256), codes(2, 16 + 256),
                codes(4, 16 + 256), codes(4, 16 + 256),
                codes(3, 16 + 128), codes(3, 16 + 128),
                codes(slots, 16), codes(slots, 16),
                pltpu.VMEM((len(MERGED), PLANE, 16, LANES), jnp.int16),
                pltpu.VMEM((len(MERGED), PLANE, 16, LANES), jnp.int16),
                dma, dma((len(pieces),)), dma((len(pieces),)), dma((len(pieces),)),
                dma((parts, 2)), dma((parts, 2)),
                dma((parts, 4)), dma((parts, 4)),
                dma((parts, 3)), dma((parts, 3)),
                dma((parts, slots)), dma((parts, slots)),
                dma((len(MERGED),)), dma((len(MERGED),)),
            ],
            compiler_params=pltpu.CompilerParams(
                collective_id=0, has_side_effects=True, vmem_limit_bytes=53 * 1024 * 1024
            ),
        )(
            pltpu.with_memory_space_constraint(factors.reshape(depth, basis), pltpu.HBM),
            pltpu.with_memory_space_constraint(screen, pltpu.HBM),
        )

    placed = (P(("grp", "mem"), None, None), P(("grp", "mem"), None))
    return jax.shard_map(
        on_device, mesh=mesh, in_specs=placed, out_specs=P(("grp", "mem"), None), check_vma=False
    )
```

```python
import functools

import jax
import jax.numpy as jnp
from jax import lax
from jax.experimental import pallas as pl
from jax.experimental.pallas import tpu as pltpu
from jax.sharding import PartitionSpec as P

LANES = 128
TOP = 32767.0
SIDE = 4
HEAD = 8
MESH = pl.DeviceIdType.MESH
ORDERS = ("yzx", "zxy", "xyz", "yzx", "zxy", "xyz", "wvz")
PIECES = (192, 256, 128)
MERGED = (3, 4, 5, 6)
PLANE = 2 * SIDE * SIDE - 1


def kernel(
    members, width, orders, pieces,
    x_ref, flags_ref, out_ref,
    screen_ref, both, turned, total, first_sum, second_sum,
    out_one, in_one, out_two, in_two, out_three, in_three, out_four, in_four, out_plane, in_plane,
    flag_sem, load_sem, pair_send, pair_recv, one_send, one_recv, two_send, two_recv,
    three_send, three_recv, four_send, four_recv, plane_send, plane_recv,
):
    depth, basis = x_ref.shape
    own = out_ref.shape[0]
    half = basis // 2
    parts = len(orders)
    occ_blocks = screen_ref.shape[1]
    grp, mem = lax.axis_index("grp"), lax.axis_index("mem")
    at = {"y": lax.div(grp, 2), "c": lax.rem(grp, 2), "x": lax.div(mem, SIDE), "z": lax.rem(mem, SIDE)}
    core = at["c"]

    at["w"] = (1 - core) * at["y"] + core * at["x"]
    at["v"] = core * at["y"] + (1 - core) * at["x"]

    def place(axis, d):
        return lax.rem(at[axis] + d, SIDE)

    def device(axis, d, flip=0):
        return moved([(axis, d)], flip)

    def moved(moves, flip=0):
        there = dict(at)
        for axis, d in moves:
            if d and axis in "wv":
                to = place(axis, d)
                on_y = 1 - core if axis == "w" else core
                there["y"] = on_y * to + (1 - on_y) * there["y"]
                there["x"] = (1 - on_y) * to + on_y * there["x"]
            elif d:
                there[axis] = place(axis, d)
        if flip:
            there["c"] = 1 - core
        return (there["y"] * 2 + there["c"], there["x"] * SIDE + there["z"])

    last_axes = sorted({order[2] for order in orders})
    peers = [device("x", 0, 1)]
    for axis in "xyz":
        for d in range(1, SIDE):
            peers.append(device(axis, d))
            if axis in last_axes:
                peers.append(device(axis, d, 1))
    barrier = pltpu.get_barrier_semaphore()
    for other in peers:
        pl.semaphore_signal(barrier, inc=1, device_id=other, device_id_type=MESH)

    starts = [sum(pieces[:n]) for n in range(len(pieces) + 1)]
    flags = pltpu.make_async_copy(flags_ref, screen_ref, flag_sem)
    flags.start()
    loads = []
    for n in range(len(pieces)):
        rows = pl.ds(starts[n], pieces[n])
        loads.append(pltpu.make_async_copy(x_ref.at[rows], both.at[rows], load_sem.at[n]))
        loads[-1].start()

    total_rows = total.shape[1]
    for p in range(parts):
        total[p, basis:total_rows, :] = jnp.zeros((total_rows - basis, LANES), jnp.float32)
        tail = second_sum.shape[1]
        second_sum[p, tail - 16 : tail, :] = jnp.zeros((16, LANES), jnp.float32)
        first_sum[p, 448:464, :] = jnp.zeros((16, LANES), jnp.float32)

    def mask(j, carry):
        rows = pl.ds(pl.multiple_of(j * width, width), width)
        keep = screen_ref[0, lax.rem(j, occ_blocks)].astype(jnp.float32)
        both[rows, :] = both[rows, :] * jnp.full((width, basis), keep, jnp.float32).astype(both.dtype)
        return carry

    pair = []
    partner = device("x", 0, 1)
    flags.wait()
    for n in range(len(pieces)):
        loads[n].wait()
        lax.fori_loop(starts[n] // width, starts[n + 1] // width, mask, 0)
    for n in range(len(pieces)):
        if n == 0:
            pl.semaphore_wait(barrier, len(peers))
        pair.append(
            pltpu.make_async_remote_copy(
                src_ref=both.at[pl.ds(starts[n], pieces[n])],
                dst_ref=both.at[pl.ds(depth + starts[n], pieces[n])],
                send_sem=pair_send.at[n], recv_sem=pair_recv.at[n],
                device_id=partner, device_id_type=MESH,
            )
        )
        pair[-1].start()

    def turn(low, high):
        def one(m, carry):
            rows = pl.ds(pl.multiple_of(m * 256, 256), 256)
            for k in range(low, high, LANES):
                turned[rows, k : k + LANES] = both[k : k + LANES, rows].T
            return carry

        lax.fori_loop(0, basis // 256, one, 0)

    def multiply(tiles, low, high, fresh):
        tall = basis // 2
        columns = pl.ds(pl.multiple_of(core * half + tiles[0] * LANES, LANES), len(tiles) * LANES)

        def one(m, carry):
            rows = pl.ds(pl.multiple_of(m * tall, LANES), tall)
            value = jnp.dot(turned[rows, low:high], both[low:high, columns], preferred_element_type=jnp.float32)
            for n, p in enumerate(tiles):
                mine = value[:, n * LANES : (n + 1) * LANES]
                total[p, rows, :] = mine if fresh else total[p, rows, :] + mine
            return carry

        lax.fori_loop(0, 2, one, 0)

    def exponent(top):
        return jnp.floor(jnp.log(jnp.maximum(top, 1e-33)) * 1.4426950408889634) + 1.0

    def coded(value, power):
        return jnp.round(value * (jnp.exp2(-power) * TOP)).astype(jnp.int32).astype(jnp.int16)

    def put(ref, values):
        rows = lax.broadcasted_iota(jnp.int32, (HEAD, LANES), 0)
        head = jnp.zeros((HEAD, LANES), jnp.float32)
        end = sum(value.shape[0] for value in values)
        for g, value in enumerate(values):
            power = exponent(jnp.max(jnp.abs(value), axis=0, keepdims=True))
            n = value.shape[0]
            ref[g * n : (g + 1) * n, :] = coded(value, power)
            head = jnp.where(rows == g, power, head)
        ref[end : end + HEAD, :] = head.astype(jnp.int32).astype(jnp.int16)

    def powers(ref, end):
        return jnp.exp2(ref[end : end + HEAD, :].astype(jnp.int32).astype(jnp.float32)) * (1.0 / TOP)

    def get(ref, scale, g, n):
        return ref[g * n : (g + 1) * n, :].astype(jnp.int32).astype(jnp.float32) * scale[g : g + 1, :]

    def group_rows(order):
        return 128 if order[0] == "z" else 112

    def load(p, order, block, c, g):
        if order[0] == "y":
            start = block * (8 * own * SIDE) + c * (4 * own * SIDE) + g * 112
            return total[p, pl.ds(pl.multiple_of(start, 8), 112), :]
        if order[0] in "xw":
            near, far = own * SIDE, 8 * own * SIDE
            if order[0] == "w":
                near, far = core * near + (1 - core) * far, (1 - core) * near + core * far
            starts = [(2 * g + n) * far + c * (4 * own * SIDE) + block * near for n in range(2)]
            return jnp.concatenate([total[p, pl.ds(pl.multiple_of(s, 8), 56), :] for s in starts], axis=0)
        starts = [
            (2 * g + n) * (8 * own * SIDE) + c * (4 * own * SIDE) + m * (own * SIDE) + block * own
            for n in range(2) for m in range(SIDE)
        ]
        return jnp.concatenate([total[p, pl.ds(s, 16), :] for s in starts], axis=0)

    def second_block(p, order, j):
        if order[1] == "z":
            starts = [c * (4 * own * SIDE) + m * (own * SIDE) + j * own for c in range(2) for m in range(SIDE)]
            return jnp.concatenate([first_sum[p, pl.ds(s, 16), :] for s in starts], axis=0)
        if order[0] != "z" or order[1] == "y":
            n = 64 if order[0] == "z" else 56
            starts = [c * 4 * n + j * n for c in range(2)]
        else:
            n = 16
            starts = [c * 256 + m * 64 + j * n for c in range(2) for m in range(SIDE)]
        return jnp.concatenate([first_sum[p, pl.ds(pl.multiple_of(s, 8), n), :] for s in starts], axis=0)

    def copy(here, there, a, b, to):
        return pltpu.make_async_remote_copy(
            src_ref=here, dst_ref=there, send_sem=a, recv_sem=b, device_id=to, device_id_type=MESH,
        )

    def sized(order, groups):
        return pl.ds(0, HEAD + groups * group_rows(order))

    def copy_one(p, s):
        order = orders[p]
        run = sized(order, 2)
        return copy(out_one.at[p, s, run], in_one.at[p, s, run], one_send.at[p, s], one_recv.at[p, s],
                    device(order[0], (1, 3)[s]))

    def copy_two(p, s, late):
        order = orders[p]
        run = sized(order, 2)
        n = 2 * s + late
        return copy(out_two.at[p, n, run], in_two.at[p, n, run], two_send.at[p, n], two_recv.at[p, n],
                    device(order[0], (1, 3)[s]))

    def second_rows(order):
        return 128 if "z" in order[:2] else 112

    def copy_three(p, d):
        order = orders[p]
        run = pl.ds(0, HEAD + second_rows(order))
        return copy(out_three.at[p, d - 1, run], in_three.at[p, d - 1, run], three_send.at[p, d - 1],
                    three_recv.at[p, d - 1], device(order[1], d))

    def copy_four(p, d, flip):
        s = 2 * d + flip - 1
        return copy(out_four.at[p, s], in_four.at[p, s], four_send.at[p, s], four_recv.at[p, s],
                    device(orders[p][2], d, flip))

    def step_one(p):
        order = orders[p]
        block = place(order[0], 2)
        for s in range(2):
            put(out_one.at[p, s], [load(p, order, block, s, g) for g in range(2)])
            copy_one(p, s).start()

    def step_solo(p):
        order = orders[p]
        for s in range(2):
            block = place(order[0], (1, 3)[s])
            put(out_two.at[p, 2 * s], [load(p, order, block, 1 - s, g) for g in range(2)])
            copy_two(p, s, 0).start()

    def step_two(p):
        order = orders[p]
        n = group_rows(order)
        for s in range(2):
            copy_one(p, s).wait_recv()
            block = place(order[0], (1, 3)[s])
            ref = in_one.at[p, s]
            scale = powers(ref, 2 * n)
            put(out_two.at[p, 2 * s + 1], [load(p, order, block, s, g) + get(ref, scale, g, n) for g in range(2)])
            copy_two(p, s, 1).start()

    def collect(p):
        order = orders[p]
        n = group_rows(order)
        for s in range(2):
            for late in range(2):
                copy_two(p, s, late).wait_recv()
        for c in range(2):
            refs = [in_two.at[p, 2 * s + (1 if c == s else 0)] for s in range(2)]
            scales = [powers(ref, 2 * n) for ref in refs]
            for g in range(2):
                value = load(p, order, at[order[0]], c, g)
                for ref, scale in zip(refs, scales):
                    value = value + get(ref, scale, g, n)
                first_sum[p, (2 * c + g) * n : (2 * c + g + 1) * n, :] = value

    def plane_rows(order, c, u, v):
        if order[0] == "z":
            steps = {"y": SIDE * 16, "x": 16} if order[1] == "y" else {"x": 16, "y": SIDE * 16}
            return pl.ds(pl.multiple_of(c * 256 + u * steps[order[1]] + v * steps[order[2]], 8), 16)
        step = own if order[1] == "z" else own * SIDE
        other = own * SIDE if order[1] == "z" else own
        return pl.ds(c * (4 * own * SIDE) + u * step + v * other, 16)

    def plane_slot(du, dv, flip):
        return (du * SIDE + dv) * 2 + flip - 1

    def step_plane(q):
        p = merged[q]
        order = orders[p]
        collect(p)
        row = lax.rem(lax.broadcasted_iota(jnp.int32, (SIDE * 16, LANES), 0), 16)
        for du in (2, 1, 3, 0):
            u = place(order[1], du)
            for flip in range(2):
                c = 1 - core if flip else core
                value = jnp.concatenate(
                    [first_sum[p, plane_rows(order, c, u, place(order[2], dv)), :] for dv in range(SIDE)], axis=0
                )
                power = exponent(jnp.max(jnp.abs(value), axis=0, keepdims=True))
                code = jnp.where(row == own, power, jnp.round(value * (jnp.exp2(-power) * TOP)))
                code = code.astype(jnp.int32).astype(jnp.int16)
                for dv in (2, 1, 3, 0):
                    if du or dv or flip:
                        n = plane_slot(du, dv, flip)
                        out_plane[q, n] = code[dv * 16 : (dv + 1) * 16, :]
                        copy(out_plane.at[q, n], in_plane.at[q, n], plane_send.at[q], plane_recv.at[q],
                             moved([(order[1], du), (order[2], dv)], flip)).start()

    def wait_plane(q, sent):
        whole = copy(out_plane.at[q], in_plane.at[q], plane_send.at[q], plane_recv.at[q], partner)
        whole.wait_send() if sent else whole.wait_recv()

    def end_plane(q):
        p = merged[q]
        order = orders[p]
        wait_plane(q, False)
        for flip in range(2):
            c = 1 - core if flip else core
            value = None
            if not flip:
                value = first_sum[p, plane_rows(order, core, at[order[1]], at[order[2]]), :]
            for du in range(SIDE):
                for dv in range(SIDE):
                    if du or dv or flip:
                        code = in_plane[q, plane_slot(du, dv, flip)].astype(jnp.int32).astype(jnp.float32)
                        term = code * (jnp.exp2(code[own : own + 1, :]) * (1.0 / TOP))
                        value = term if value is None else value + term
            columns = pl.ds(pl.multiple_of(c * half + p * LANES, LANES), LANES)
            out_ref[:, columns] = value[0:own, :]

    def step_three(p):
        order = orders[p]
        collect(p)
        for d in range(1, SIDE):
            put(out_three.at[p, d - 1], [second_block(p, order, place(order[1], d))])
            copy_three(p, d).start()

    def last_rows(order, c, k):
        if "z" in order[:2]:
            return pl.ds(pl.multiple_of(c * 64 + k * 16, 8), 16)
        return pl.ds(c * 4 * own + k * own, 16)

    def step_four(p):
        order = orders[p]
        n = second_rows(order)
        value = second_block(p, order, at[order[1]])
        for d in range(1, SIDE):
            copy_three(p, d).wait_recv()
            ref = in_three.at[p, d - 1]
            value = value + get(ref, powers(ref, n), 0, n)
        second_sum[p, 0:n, :] = value
        rows = lax.broadcasted_iota(jnp.int32, (16, LANES), 0)
        for d in range(SIDE):
            for flip in range(2):
                if d or flip:
                    c = 1 - core if flip else core
                    value = second_sum[p, last_rows(order, c, place(order[2], d)), :]
                    top = jnp.max(jnp.where(rows < own, jnp.abs(value), 0.0), axis=0, keepdims=True)
                    power = exponent(top)
                    code = jnp.round(value * (jnp.exp2(-power) * TOP))
                    code = jnp.where(rows < own, code, power)
                    out_four[p, 2 * d + flip - 1] = code.astype(jnp.int32).astype(jnp.int16)
                    copy_four(p, d, flip).start()

    def step_five(p):
        order = orders[p]
        for flip in range(2):
            c = 1 - core if flip else core
            value = None
            if not flip:
                value = second_sum[p, last_rows(order, core, at[order[2]]), :]
            for d in range(SIDE):
                if d or flip:
                    copy_four(p, d, flip).wait_recv()
                    code = in_four[p, 2 * d + flip - 1].astype(jnp.int32).astype(jnp.float32)
                    term = code * (jnp.exp2(code[own : own + 1, :]) * (1.0 / TOP))
                    value = term if value is None else value + term
            columns = pl.ds(pl.multiple_of(c * half + p * LANES, LANES), LANES)
            out_ref[:, columns] = value[0:own, :]

    first, rest = [0, 1, 2], [[3, 4, 5, 6]]
    merged = MERGED
    apart = [p for p in range(parts) if p not in merged]
    edges = [depth // LANES * LANES] + [depth + start for start in starts[1:]]
    turn(0, edges[0])
    multiply(first, 0, edges[0], True)
    pair[0].wait_recv()
    turn(edges[0], edges[1])
    multiply(first, edges[0], edges[1], False)
    for n in range(1, len(pieces)):
        pair[n].wait_recv()
        turn(edges[n], edges[n + 1])
    multiply(first, edges[1], 2 * depth, False)
    for p in first:
        step_one(p)
    for p in first:
        step_solo(p)
    late = rest[0]
    multiply(late, 0, 2 * depth, True)
    for p in late:
        step_one(p)
    for p in first:
        step_two(p)
    for p in late[:-1]:
        step_solo(p)
    for p in late[:-1]:
        step_two(p)
    step_solo(late[-1])
    step_two(late[-1])
    for p in first:
        step_three(p)
    for q in (1, 0, 2, 3):
        step_plane(q)
    for p in apart:
        step_four(p)
    for n in range(len(pieces)):
        pair[n].wait_send()
    for p in range(parts):
        for s in range(2):
            copy_one(p, s).wait_send()
            for late_half in range(2):
                copy_two(p, s, late_half).wait_send()
    for p in apart:
        for d in range(1, SIDE):
            copy_three(p, d).wait_send()
    for q in (1, 0, 2, 3):
        end_plane(q)
    for p in apart:
        step_five(p)
    for q in range(len(merged)):
        wait_plane(q, True)
    for p in apart:
        for d in range(SIDE):
            for flip in range(2):
                if d or flip:
                    copy_four(p, d, flip).wait_send()


def solution(mesh):
    groups, members = mesh.shape["grp"], mesh.shape["mem"]

    def on_device(factors, screen):
        aux_rows, occ_count, basis = factors.shape
        depth = aux_rows * occ_count
        own = basis // (groups * members)
        parts = basis // 2 // LANES
        pieces = PIECES
        dma = pltpu.SemaphoreType.DMA
        vmem = pl.BlockSpec(memory_space=pltpu.VMEM)
        slots = 2 * SIDE - 1

        def codes(count, rows):
            return pltpu.VMEM((parts, count, rows, LANES), jnp.int16)

        return pl.pallas_call(
            functools.partial(kernel, members, occ_count // screen.shape[1], ORDERS, pieces),
            out_shape=jax.ShapeDtypeStruct((own, basis), jnp.float32),
            in_specs=[pl.BlockSpec(memory_space=pltpu.HBM)] * 2,
            out_specs=vmem,
            scratch_shapes=[
                pltpu.SMEM(screen.shape, jnp.int32),
                pltpu.VMEM((2 * depth, basis), jnp.bfloat16),
                pltpu.VMEM((basis, 2 * depth), jnp.bfloat16),
                pltpu.VMEM((parts, basis + 8, LANES), jnp.float32),
                pltpu.VMEM((parts, 512, LANES), jnp.float32),
                pltpu.VMEM((parts, 128, LANES), jnp.float32),
                codes(2, 16 + 256), codes(2, 16 + 256),
                codes(4, 16 + 256), codes(4, 16 + 256),
                codes(3, 16 + 128), codes(3, 16 + 128),
                codes(slots, 16), codes(slots, 16),
                pltpu.VMEM((len(MERGED), PLANE, 16, LANES), jnp.int16),
                pltpu.VMEM((len(MERGED), PLANE, 16, LANES), jnp.int16),
                dma, dma((len(pieces),)), dma((len(pieces),)), dma((len(pieces),)),
                dma((parts, 2)), dma((parts, 2)),
                dma((parts, 4)), dma((parts, 4)),
                dma((parts, 3)), dma((parts, 3)),
                dma((parts, slots)), dma((parts, slots)),
                dma((len(MERGED),)), dma((len(MERGED),)),
            ],
            compiler_params=pltpu.CompilerParams(
                collective_id=0, has_side_effects=True, vmem_limit_bytes=53 * 1024 * 1024
            ),
        )(
            pltpu.with_memory_space_constraint(factors.reshape(depth, basis), pltpu.HBM),
            pltpu.with_memory_space_constraint(screen, pltpu.HBM),
        )

    placed = (P(("grp", "mem"), None, None), P(("grp", "mem"), None))
    return jax.shard_map(
        on_device, mesh=mesh, in_specs=placed, out_specs=P(("grp", "mem"), None), check_vma=False
    )
```

```python
import functools

import jax
import jax.numpy as jnp
from jax import lax
from jax.experimental import pallas as pl
from jax.experimental.pallas import tpu as pltpu
from jax.sharding import PartitionSpec as P

LANES = 128
TOP = 32767.0
SIDE = 4
HEAD = 8
MESH = pl.DeviceIdType.MESH
ORDERS = ("yzx", "zxy", "xyz", "yzx", "zxy", "xyz", "wvz")
PIECES = (192, 256, 128)
MERGED = (3, 4, 5, 6)
PLANE = 2 * SIDE * SIDE - 1


def kernel(
    members, width, orders, pieces,
    x_ref, flags_ref, out_ref,
    screen_ref, both, turned, total, first_sum, second_sum,
    out_one, in_one, out_two, in_two, out_three, in_three, out_four, in_four, out_plane, in_plane,
    flag_sem, load_sem, pair_send, pair_recv, one_send, one_recv, two_send, two_recv,
    three_send, three_recv, four_send, four_recv, plane_send, plane_recv,
):
    depth, basis = x_ref.shape
    own = out_ref.shape[0]
    half = basis // 2
    parts = len(orders)
    occ_blocks = screen_ref.shape[1]
    grp, mem = lax.axis_index("grp"), lax.axis_index("mem")
    at = {"y": lax.div(grp, 2), "c": lax.rem(grp, 2), "x": lax.div(mem, SIDE), "z": lax.rem(mem, SIDE)}
    core = at["c"]

    at["w"] = (1 - core) * at["y"] + core * at["x"]
    at["v"] = core * at["y"] + (1 - core) * at["x"]

    def place(axis, d):
        return lax.rem(at[axis] + d, SIDE)

    def device(axis, d, flip=0):
        return moved([(axis, d)], flip)

    def moved(moves, flip=0):
        there = dict(at)
        for axis, d in moves:
            if d and axis in "wv":
                to = place(axis, d)
                on_y = 1 - core if axis == "w" else core
                there["y"] = on_y * to + (1 - on_y) * there["y"]
                there["x"] = (1 - on_y) * to + on_y * there["x"]
            elif d:
                there[axis] = place(axis, d)
        if flip:
            there["c"] = 1 - core
        return (there["y"] * 2 + there["c"], there["x"] * SIDE + there["z"])

    starts = [sum(pieces[:n]) for n in range(len(pieces) + 1)]
    flags = pltpu.make_async_copy(flags_ref, screen_ref, flag_sem)
    flags.start()
    loads = []
    for n in range(len(pieces)):
        rows = pl.ds(starts[n], pieces[n])
        loads.append(pltpu.make_async_copy(x_ref.at[rows], both.at[rows], load_sem.at[n]))
        loads[-1].start()

    last_axes = sorted({order[2] for order in orders})
    peers = [device("x", 0, 1)]
    for axis in "xyz":
        for d in range(1, SIDE):
            peers.append(device(axis, d))
            if axis in last_axes:
                peers.append(device(axis, d, 1))
    barrier = pltpu.get_barrier_semaphore()
    for other in peers:
        pl.semaphore_signal(barrier, inc=1, device_id=other, device_id_type=MESH)

    total_rows = total.shape[1]
    for p in range(parts):
        total[p, basis:total_rows, :] = jnp.zeros((total_rows - basis, LANES), jnp.float32)
        tail = second_sum.shape[1]
        second_sum[p, tail - 16 : tail, :] = jnp.zeros((16, LANES), jnp.float32)
        first_sum[p, 448:464, :] = jnp.zeros((16, LANES), jnp.float32)

    def mask(j, carry):
        rows = pl.ds(pl.multiple_of(j * width, width), width)
        keep = screen_ref[0, lax.rem(j, occ_blocks)].astype(jnp.float32)
        both[rows, :] = (both[rows, :].astype(jnp.float32) * keep).astype(both.dtype)
        return carry

    pair = []
    partner = device("x", 0, 1)
    flags.wait()
    for n in range(len(pieces)):
        loads[n].wait()
        lax.fori_loop(starts[n] // width, starts[n + 1] // width, mask, 0)
    for n in range(len(pieces)):
        if n == 0:
            pl.semaphore_wait(barrier, len(peers))
        pair.append(
            pltpu.make_async_remote_copy(
                src_ref=both.at[pl.ds(starts[n], pieces[n])],
                dst_ref=both.at[pl.ds(depth + starts[n], pieces[n])],
                send_sem=pair_send.at[n], recv_sem=pair_recv.at[n],
                device_id=partner, device_id_type=MESH,
            )
        )
        pair[-1].start()

    def turn(low, high):
        def one(m, carry):
            rows = pl.ds(pl.multiple_of(m * 256, 256), 256)
            for k in range(low, high, LANES):
                turned[rows, k : k + LANES] = both[k : k + LANES, rows].T
            return carry

        lax.fori_loop(0, basis // 256, one, 0)

    def multiply(tiles, low, high, fresh):
        tall = basis // 2
        columns = pl.ds(pl.multiple_of(core * half + tiles[0] * LANES, LANES), len(tiles) * LANES)

        def one(m, carry):
            rows = pl.ds(pl.multiple_of(m * tall, LANES), tall)
            value = jnp.dot(turned[rows, low:high], both[low:high, columns], preferred_element_type=jnp.float32)
            for n, p in enumerate(tiles):
                mine = value[:, n * LANES : (n + 1) * LANES]
                total[p, rows, :] = mine if fresh else total[p, rows, :] + mine
            return carry

        lax.fori_loop(0, 2, one, 0)

    def exponent(top):
        return jnp.floor(jnp.log(jnp.maximum(top, 1e-33)) * 1.4426950408889634) + 1.0

    def coded(value, power):
        return jnp.round(value * (jnp.exp2(-power) * TOP)).astype(jnp.int32).astype(jnp.int16)

    def put(ref, values):
        rows = lax.broadcasted_iota(jnp.int32, (HEAD, LANES), 0)
        head = jnp.zeros((HEAD, LANES), jnp.float32)
        end = sum(value.shape[0] for value in values)
        for g, value in enumerate(values):
            power = exponent(jnp.max(jnp.abs(value), axis=0, keepdims=True))
            n = value.shape[0]
            ref[g * n : (g + 1) * n, :] = coded(value, power)
            head = jnp.where(rows == g, power, head)
        ref[end : end + HEAD, :] = head.astype(jnp.int32).astype(jnp.int16)

    def powers(ref, end):
        return jnp.exp2(ref[end : end + HEAD, :].astype(jnp.int32).astype(jnp.float32)) * (1.0 / TOP)

    def get(ref, scale, g, n):
        return ref[g * n : (g + 1) * n, :].astype(jnp.int32).astype(jnp.float32) * scale[g : g + 1, :]

    def group_rows(order):
        return 128 if order[0] == "z" else 112

    def load(p, order, block, c, g):
        if order[0] == "y":
            start = block * (8 * own * SIDE) + c * (4 * own * SIDE) + g * 112
            return total[p, pl.ds(pl.multiple_of(start, 8), 112), :]
        if order[0] in "xw":
            near, far = own * SIDE, 8 * own * SIDE
            if order[0] == "w":
                near, far = core * near + (1 - core) * far, (1 - core) * near + core * far
            starts = [(2 * g + n) * far + c * (4 * own * SIDE) + block * near for n in range(2)]
            return jnp.concatenate([total[p, pl.ds(pl.multiple_of(s, 8), 56), :] for s in starts], axis=0)
        starts = [
            (2 * g + n) * (8 * own * SIDE) + c * (4 * own * SIDE) + m * (own * SIDE) + block * own
            for n in range(2) for m in range(SIDE)
        ]
        return jnp.concatenate([total[p, pl.ds(s, 16), :] for s in starts], axis=0)

    def second_block(p, order, j):
        if order[1] == "z":
            starts = [c * (4 * own * SIDE) + m * (own * SIDE) + j * own for c in range(2) for m in range(SIDE)]
            return jnp.concatenate([first_sum[p, pl.ds(s, 16), :] for s in starts], axis=0)
        if order[0] != "z" or order[1] == "y":
            n = 64 if order[0] == "z" else 56
            starts = [c * 4 * n + j * n for c in range(2)]
        else:
            n = 16
            starts = [c * 256 + m * 64 + j * n for c in range(2) for m in range(SIDE)]
        return jnp.concatenate([first_sum[p, pl.ds(pl.multiple_of(s, 8), n), :] for s in starts], axis=0)

    def copy(here, there, a, b, to):
        return pltpu.make_async_remote_copy(
            src_ref=here, dst_ref=there, send_sem=a, recv_sem=b, device_id=to, device_id_type=MESH,
        )

    def sized(order, groups):
        return pl.ds(0, HEAD + groups * group_rows(order))

    def copy_one(p, s):
        order = orders[p]
        run = sized(order, 2)
        return copy(out_one.at[p, s, run], in_one.at[p, s, run], one_send.at[p, s], one_recv.at[p, s],
                    device(order[0], (1, 3)[s]))

    def copy_two(p, s, late):
        order = orders[p]
        run = sized(order, 2)
        n = 2 * s + late
        return copy(out_two.at[p, n, run], in_two.at[p, n, run], two_send.at[p, n], two_recv.at[p, n],
                    device(order[0], (1, 3)[s]))

    def second_rows(order):
        return 128 if "z" in order[:2] else 112

    def copy_three(p, d):
        order = orders[p]
        run = pl.ds(0, HEAD + second_rows(order))
        return copy(out_three.at[p, d - 1, run], in_three.at[p, d - 1, run], three_send.at[p, d - 1],
                    three_recv.at[p, d - 1], device(order[1], d))

    def copy_four(p, d, flip):
        s = 2 * d + flip - 1
        return copy(out_four.at[p, s], in_four.at[p, s], four_send.at[p, s], four_recv.at[p, s],
                    device(orders[p][2], d, flip))

    def step_one(p):
        order = orders[p]
        block = place(order[0], 2)
        for s in range(2):
            put(out_one.at[p, s], [load(p, order, block, s, g) for g in range(2)])
            copy_one(p, s).start()

    def step_solo(p):
        order = orders[p]
        for s in range(2):
            block = place(order[0], (1, 3)[s])
            put(out_two.at[p, 2 * s], [load(p, order, block, 1 - s, g) for g in range(2)])
            copy_two(p, s, 0).start()

    def step_two(p):
        order = orders[p]
        n = group_rows(order)
        for s in range(2):
            copy_one(p, s).wait_recv()
            block = place(order[0], (1, 3)[s])
            ref = in_one.at[p, s]
            scale = powers(ref, 2 * n)
            put(out_two.at[p, 2 * s + 1], [load(p, order, block, s, g) + get(ref, scale, g, n) for g in range(2)])
            copy_two(p, s, 1).start()

    def collect(p):
        order = orders[p]
        n = group_rows(order)
        for s in range(2):
            for late in range(2):
                copy_two(p, s, late).wait_recv()
        for c in range(2):
            refs = [in_two.at[p, 2 * s + (1 if c == s else 0)] for s in range(2)]
            scales = [powers(ref, 2 * n) for ref in refs]
            for g in range(2):
                value = load(p, order, at[order[0]], c, g)
                for ref, scale in zip(refs, scales):
                    value = value + get(ref, scale, g, n)
                first_sum[p, (2 * c + g) * n : (2 * c + g + 1) * n, :] = value

    def plane_rows(order, c, u, v):
        if order[0] == "z":
            steps = {"y": SIDE * 16, "x": 16} if order[1] == "y" else {"x": 16, "y": SIDE * 16}
            return pl.ds(pl.multiple_of(c * 256 + u * steps[order[1]] + v * steps[order[2]], 8), 16)
        step = own if order[1] == "z" else own * SIDE
        other = own * SIDE if order[1] == "z" else own
        return pl.ds(c * (4 * own * SIDE) + u * step + v * other, 16)

    def plane_slot(du, dv, flip):
        return (du * SIDE + dv) * 2 + flip - 1

    def step_plane(q):
        p = merged[q]
        order = orders[p]
        collect(p)
        row = lax.rem(lax.broadcasted_iota(jnp.int32, (SIDE * 16, LANES), 0), 16)
        for du in (2, 1, 3, 0):
            u = place(order[1], du)
            for flip in range(2):
                c = 1 - core if flip else core
                value = jnp.concatenate(
                    [first_sum[p, plane_rows(order, c, u, place(order[2], dv)), :] for dv in range(SIDE)], axis=0
                )
                power = exponent(jnp.max(jnp.abs(value), axis=0, keepdims=True))
                code = jnp.where(row == own, power, jnp.round(value * (jnp.exp2(-power) * TOP)))
                code = code.astype(jnp.int32).astype(jnp.int16)
                for dv in (2, 1, 3, 0):
                    if du or dv or flip:
                        n = plane_slot(du, dv, flip)
                        out_plane[q, n] = code[dv * 16 : (dv + 1) * 16, :]
                        copy(out_plane.at[q, n], in_plane.at[q, n], plane_send.at[q], plane_recv.at[q],
                             moved([(order[1], du), (order[2], dv)], flip)).start()

    def wait_plane(q, sent):
        whole = copy(out_plane.at[q], in_plane.at[q], plane_send.at[q], plane_recv.at[q], partner)
        whole.wait_send() if sent else whole.wait_recv()

    def end_plane(q):
        p = merged[q]
        order = orders[p]
        wait_plane(q, False)
        for flip in range(2):
            c = 1 - core if flip else core
            value = None
            if not flip:
                value = first_sum[p, plane_rows(order, core, at[order[1]], at[order[2]]), :]
            for du in range(SIDE):
                for dv in range(SIDE):
                    if du or dv or flip:
                        code = in_plane[q, plane_slot(du, dv, flip)].astype(jnp.int32).astype(jnp.float32)
                        term = code * (jnp.exp2(code[own : own + 1, :]) * (1.0 / TOP))
                        value = term if value is None else value + term
            columns = pl.ds(pl.multiple_of(c * half + p * LANES, LANES), LANES)
            out_ref[:, columns] = value[0:own, :]

    def step_three(p):
        order = orders[p]
        collect(p)
        for d in range(1, SIDE):
            put(out_three.at[p, d - 1], [second_block(p, order, place(order[1], d))])
            copy_three(p, d).start()

    def last_rows(order, c, k):
        if "z" in order[:2]:
            return pl.ds(pl.multiple_of(c * 64 + k * 16, 8), 16)
        return pl.ds(c * 4 * own + k * own, 16)

    def step_four(p):
        order = orders[p]
        n = second_rows(order)
        value = second_block(p, order, at[order[1]])
        for d in range(1, SIDE):
            copy_three(p, d).wait_recv()
            ref = in_three.at[p, d - 1]
            value = value + get(ref, powers(ref, n), 0, n)
        second_sum[p, 0:n, :] = value
        rows = lax.broadcasted_iota(jnp.int32, (16, LANES), 0)
        for d in range(SIDE):
            for flip in range(2):
                if d or flip:
                    c = 1 - core if flip else core
                    value = second_sum[p, last_rows(order, c, place(order[2], d)), :]
                    top = jnp.max(jnp.where(rows < own, jnp.abs(value), 0.0), axis=0, keepdims=True)
                    power = exponent(top)
                    code = jnp.round(value * (jnp.exp2(-power) * TOP))
                    code = jnp.where(rows < own, code, power)
                    out_four[p, 2 * d + flip - 1] = code.astype(jnp.int32).astype(jnp.int16)
                    copy_four(p, d, flip).start()

    def step_five(p):
        order = orders[p]
        for flip in range(2):
            c = 1 - core if flip else core
            value = None
            if not flip:
                value = second_sum[p, last_rows(order, core, at[order[2]]), :]
            for d in range(SIDE):
                if d or flip:
                    copy_four(p, d, flip).wait_recv()
                    code = in_four[p, 2 * d + flip - 1].astype(jnp.int32).astype(jnp.float32)
                    term = code * (jnp.exp2(code[own : own + 1, :]) * (1.0 / TOP))
                    value = term if value is None else value + term
            columns = pl.ds(pl.multiple_of(c * half + p * LANES, LANES), LANES)
            out_ref[:, columns] = value[0:own, :]

    first, rest = [0, 1, 2], [[3, 4, 5, 6]]
    merged = MERGED
    apart = [p for p in range(parts) if p not in merged]
    edges = [depth // LANES * LANES] + [depth + start for start in starts[1:]]
    turn(0, edges[0])
    multiply(first, 0, edges[0], True)
    pair[0].wait_recv()
    turn(edges[0], edges[1])
    multiply(first, edges[0], edges[1], False)
    for n in range(1, len(pieces)):
        pair[n].wait_recv()
        turn(edges[n], edges[n + 1])
    multiply(first, edges[1], 2 * depth, False)
    for p in first:
        step_one(p)
    for p in first:
        step_solo(p)
    late = rest[0]
    multiply(late, 0, 2 * depth, True)
    for p in late:
        step_one(p)
    for p in first:
        step_two(p)
    for p in late[:-1]:
        step_solo(p)
    for p in late[:-1]:
        step_two(p)
    step_solo(late[-1])
    step_two(late[-1])
    for p in first:
        step_three(p)
    for q in (1, 0, 2, 3):
        step_plane(q)
    for p in apart:
        step_four(p)
    for n in range(len(pieces)):
        pair[n].wait_send()
    for p in range(parts):
        for s in range(2):
            copy_one(p, s).wait_send()
            for late_half in range(2):
                copy_two(p, s, late_half).wait_send()
    for p in apart:
        for d in range(1, SIDE):
            copy_three(p, d).wait_send()
    for q in (1, 0, 2, 3):
        end_plane(q)
    for p in apart:
        step_five(p)
    for q in range(len(merged)):
        wait_plane(q, True)
    for p in apart:
        for d in range(SIDE):
            for flip in range(2):
                if d or flip:
                    copy_four(p, d, flip).wait_send()


def solution(mesh):
    groups, members = mesh.shape["grp"], mesh.shape["mem"]

    def on_device(factors, screen):
        aux_rows, occ_count, basis = factors.shape
        depth = aux_rows * occ_count
        own = basis // (groups * members)
        parts = basis // 2 // LANES
        pieces = PIECES
        dma = pltpu.SemaphoreType.DMA
        vmem = pl.BlockSpec(memory_space=pltpu.VMEM)
        slots = 2 * SIDE - 1

        def codes(count, rows):
            return pltpu.VMEM((parts, count, rows, LANES), jnp.int16)

        return pl.pallas_call(
            functools.partial(kernel, members, occ_count // screen.shape[1], ORDERS, pieces),
            out_shape=jax.ShapeDtypeStruct((own, basis), jnp.float32),
            in_specs=[pl.BlockSpec(memory_space=pltpu.HBM)] * 2,
            out_specs=vmem,
            scratch_shapes=[
                pltpu.SMEM(screen.shape, jnp.int32),
                pltpu.VMEM((2 * depth, basis), jnp.bfloat16),
                pltpu.VMEM((basis, 2 * depth), jnp.bfloat16),
                pltpu.VMEM((parts, basis + 8, LANES), jnp.float32),
                pltpu.VMEM((parts, 512, LANES), jnp.float32),
                pltpu.VMEM((parts, 128, LANES), jnp.float32),
                codes(2, 16 + 256), codes(2, 16 + 256),
                codes(4, 16 + 256), codes(4, 16 + 256),
                codes(3, 16 + 128), codes(3, 16 + 128),
                codes(slots, 16), codes(slots, 16),
                pltpu.VMEM((len(MERGED), PLANE, 16, LANES), jnp.int16),
                pltpu.VMEM((len(MERGED), PLANE, 16, LANES), jnp.int16),
                dma, dma((len(pieces),)), dma((len(pieces),)), dma((len(pieces),)),
                dma((parts, 2)), dma((parts, 2)),
                dma((parts, 4)), dma((parts, 4)),
                dma((parts, 3)), dma((parts, 3)),
                dma((parts, slots)), dma((parts, slots)),
                dma((len(MERGED),)), dma((len(MERGED),)),
            ],
            compiler_params=pltpu.CompilerParams(
                collective_id=0, has_side_effects=True, vmem_limit_bytes=53 * 1024 * 1024
            ),
        )(
            pltpu.with_memory_space_constraint(factors.reshape(depth, basis), pltpu.HBM),
            pltpu.with_memory_space_constraint(screen, pltpu.HBM),
        )

    placed = (P(("grp", "mem"), None, None), P(("grp", "mem"), None))
    return jax.shard_map(
        on_device, mesh=mesh, in_specs=placed, out_specs=P(("grp", "mem"), None), check_vma=False
    )
```
